512 devices in a mesh: gx: 8 (over y), gy: 64 (over x, z, core).
Axes of the slice: x: 4, y: 8, z: 8, core: 2. Of those that a mesh axis runs over, the one named last changes fastest.
Arguments:
- basis_mats: float32 [12, 275, 275], replicated, may hold values from -8 to 8.5, as said below
- coeffs: float32 [8192, 12], P(('gx', 'gy')), may hold values from 0.5 to 2
- element_loads: float32 [8192, 275], P(('gx', 'gy')), may hold values from -18 to 18
- elem_faces: int32 [8192, 6], P(('gx', 'gy')), may hold values from 0 to 71, as said below
- orient_codes: int32 [8192, 6], P(('gx', 'gy')), may hold values from 0 to 7
- shared_owned: int32 [512, 2, 4], P(('gx', 'gy')), may hold values from 0 to 63, as said below
- shared_remote: int32 [512, 2, 4], P(('gx', 'gy')), may hold values from 0 to 7, as said below
- lower_peers: int32 [512, 2], P(('gx', 'gy')), may hold values from 0 to 511, as said below
- upper_peers: int32 [512, 2], P(('gx', 'gy')), may hold values from 0 to 511, as said below
Outputs:
- trace: float32 [25, 32768], P(None, ('gx', 'gy'))
- residual: float32 [25, 32768], P(None, ('gx', 'gy'))
The draws below stay inside these ranges and needn't reach their ends.
Inputs may be any that keep to these rules, and one draw needn't show every extreme that they name: `basis_mats`: each matrix is symmetric with every eigenvalue at least 0.5. `elem_faces`: an entry below 64 is a face slot that the element's device owns; an entry 64 + r is that device's remote slot r. Every owned slot of a device is named by one or two of its element faces, every remote slot by exactly one. `shared_owned`: row (d, i) lists 4 distinct owned slots of device d, in message order, that device lower_peers[d, i] uses; the two rows of a device are disjoint. `shared_remote`: row (d, i) lists remote slots of device d in message order: its k-th entry is the face that device upper_peers[d, i] lists k-th in its row i of shared_owned. The two rows of a device together hold each of its 8 remote slots once. upper_peers[lower_peers[d, i], i] = d for every device d and i; the two entries of a row differ. Peers are arbitrary device numbers. lower_peers[upper_peers[d, i], i] = d for every device d and i; the two entries of a row differ; each column is a permutation of the devices. Peers are arbitrary device numbers.
All inputs are finite; a program needn't handle non-finite values.
Results may differ from the reference program's by a relative error of at most 0.0003.
Values sent between devices are 32-bit elements; how exact they have to be, the bound alone decides.
No kernel may reach another device: no remote copies, remote signals or barrier semaphores. Data moves between devices by JAX's collectives and lax.ppermute only.
A program may use at most 128 MiB of HBM per device.

```python
import math
import jax
import jax.numpy as jnp
import numpy as np
from jax import lax

SIDE = 5
FACE_DOFS = 25
CELL_DOFS = 125
TRACE_DOFS = 150
LOCAL_DOFS = 275
TERMS = 12
EX = 4
EY = 4
EZ = 1
ITERS = 4
ELEM_DEV = 16
FACE_DEV = 64
SHARED = 4
REMOTE = 8
ELEMS = 8192
N_GX = 8
N_GY = 64


def canonical_faces():
    cells = EX * EY * EZ
    plane = EX * EY * EZ
    layout_table = np.zeros((cells, 6), np.int32)
    for first_axis in range(EX):
        for second_axis in range(EY):
            for third_axis in range(EZ):
                cell_index = (first_axis * EY + second_axis) * EZ + third_axis
                layout_table[cell_index, 0] = (first_axis * EY + second_axis) * EZ + third_axis
                if first_axis + 1 < EX:
                    layout_table[cell_index, 1] = ((first_axis + 1) * EY + second_axis) * EZ + third_axis
                else:
                    layout_table[cell_index, 1] = FACE_DEV + second_axis * EZ + third_axis
                layout_table[cell_index, 2] = plane + (second_axis * EX + first_axis) * EZ + third_axis
                if second_axis + 1 < EY:
                    layout_table[cell_index, 3] = plane + ((second_axis + 1) * EX + first_axis) * EZ + third_axis
                else:
                    layout_table[cell_index, 3] = FACE_DEV + SHARED + first_axis * EZ + third_axis
                layout_table[cell_index, 4] = 2 * plane + (third_axis * EX + first_axis) * EY + second_axis
                layout_table[cell_index, 5] = 2 * plane + ((third_axis + 1) * EX + first_axis) * EY + second_axis
    return layout_table


def per_device_orders(key, devices, length):
    sub_keys = jax.random.split(key, devices)
    return jax.vmap(lambda sub_key: jax.random.permutation(sub_key, length))(sub_keys).astype(jnp.int32)


def layout(key):
    devices = N_GX * N_GY
    cells = EX * EY * EZ
    placed = jax.random.permutation(jax.random.fold_in(key, 101), devices).astype(jnp.int32)
    blocks = jnp.argsort(placed).astype(jnp.int32)
    block_row = blocks // N_GY
    block_col = blocks % N_GY
    lower = jnp.stack([placed[(block_row - 1) % N_GX * N_GY + block_col], placed[block_row * N_GY + (block_col - 1) % N_GY]], axis=1)
    upper = jnp.stack([placed[(block_row + 1) % N_GX * N_GY + block_col], placed[block_row * N_GY + (block_col + 1) % N_GY]], axis=1)
    cell_order = per_device_orders(jax.random.fold_in(key, 102), devices, cells)
    owned_order = per_device_orders(jax.random.fold_in(key, 103), devices, FACE_DEV)
    remote_order = per_device_orders(jax.random.fold_in(key, 104), devices, REMOTE)
    canon = jnp.asarray(canonical_faces())
    owned_pick = owned_order[:, jnp.minimum(canon, FACE_DEV - 1)]
    remote_pick = remote_order[:, jnp.clip(canon - FACE_DEV, 0, REMOTE - 1)]
    slots = jnp.where(canon[None] < FACE_DEV, owned_pick, FACE_DEV + remote_pick)
    inverse = jnp.argsort(cell_order, axis=1).astype(jnp.int32)
    stored = jnp.take_along_axis(slots, inverse[:, :, None], axis=1)
    plane = EX * EY * EZ
    owned_lists = jnp.stack([owned_order[:, :SHARED], owned_order[:, plane:plane + SHARED]], axis=1)
    remote_lists = remote_order.reshape(devices, 2, SHARED)
    return (stored.reshape(devices * cells, 6).astype(jnp.int32), owned_lists, remote_lists, lower.astype(jnp.int32), upper.astype(jnp.int32))


def draw_basis_mats(key, part):
    entries = jnp.clip(jax.random.normal(key, (TERMS, LOCAL_DOFS, LOCAL_DOFS), jnp.float32), -4.0, 4.0)
    gram_part = jnp.einsum('kab,kcb->kac', entries, entries, precision=lax.Precision.HIGHEST) / (2.0 * LOCAL_DOFS)
    return gram_part + 0.5 * jnp.eye(LOCAL_DOFS, dtype=jnp.float32)[None]


def draw_elem_faces(key, part):
    return layout(key)[0]


def draw_shared_owned(key, part):
    return layout(key)[1]


def draw_shared_remote(key, part):
    return layout(key)[2]


def draw_lower_peers(key, part):
    return layout(key)[3]


def draw_upper_peers(key, part):
    return layout(key)[4]


def set_ends(array, key, least, largest):
    place = [jax.random.randint(jax.random.fold_in(key, axis), (), 0, length) for axis, length in enumerate(array.shape)]
    main_axis = array.shape.index(max(array.shape))
    next_to = place[:main_axis] + [(place[main_axis] + 1) % array.shape[main_axis]] + place[main_axis + 1:]
    return array.at[tuple(place)].set(least).at[tuple(next_to)].set(largest)


def steps_of(stream_key, shape, cuts, smallest, top_value):
    def one(axis_at, blocks):
        steps = jax.random.uniform(jax.random.fold_in(jax.random.fold_in(stream_key, 6), axis_at), (blocks,), jnp.float32, smallest / len(cuts), top_value / len(cuts))
        return jnp.repeat(jnp.exp(steps), shape[axis_at] // blocks).reshape((-1,) + (1,) * (len(shape) - axis_at - 1))

    gain = one(*cuts[0])
    for cut in cuts[1:]:
        gain = gain * one(*cut)
    return gain


def bell_draw(own_key, dims, deviation, limit, shards=(), held_as=jnp.bfloat16):
    drawn = jax.random.normal(own_key, dims, jnp.float32) * deviation
    if len(shards) > 0:
        drawn = steps_of(own_key, dims, shards, -0.22, 0.18) * drawn
    return jnp.clip(drawn, min=-limit, max=limit).astype(held_as)


def setup_inputs(seed: int = 0) -> dict:
    arg_keys = jax.random.split(jax.random.key(seed), 10)
    return {
        "basis_mats": draw_basis_mats(jax.random.fold_in(arg_keys[9], 71), 0),
        "coeffs": jnp.clip(jnp.exp(math.log(2.0) - 1.3862944 * jax.random.uniform(arg_keys[1], (ELEMS, TERMS), jnp.float32) ** steps_of(arg_keys[1], (ELEMS, TERMS), ((0, 512),), -0.2, 0.2)), 0.5, 2.0),
        "element_loads": bell_draw(arg_keys[2], (ELEMS, LOCAL_DOFS), 3.0, 18.0, ((0, 512),), jnp.float32),
        "elem_faces": draw_elem_faces(jax.random.fold_in(arg_keys[9], 71), 0),
        "orient_codes": set_ends(jax.random.randint(arg_keys[4], (ELEMS, 6), 0, 8), jax.random.fold_in(arg_keys[4], 1), 0, 7).astype(jnp.int32),
        "shared_owned": draw_shared_owned(jax.random.fold_in(arg_keys[9], 71), 0),
        "shared_remote": draw_shared_remote(jax.random.fold_in(arg_keys[9], 71), 0),
        "lower_peers": draw_lower_peers(jax.random.fold_in(arg_keys[9], 71), 0),
        "upper_peers": draw_upper_peers(jax.random.fold_in(arg_keys[9], 71), 0),
    }


full_precision = lax.Precision.HIGHEST

def orient_table():
    edge_nodes = SIDE
    codes_table = np.zeros((8, edge_nodes * edge_nodes), np.int32)
    for code_index in range(8):
        for first_axis in range(edge_nodes):
            for second_axis in range(edge_nodes):
                if code_index & 1:
                    first_new, second_new = (second_axis, first_axis)
                else:
                    first_new, second_new = (first_axis, second_axis)
                if code_index & 2:
                    first_new = edge_nodes - 1 - first_new
                if code_index & 4:
                    second_new = edge_nodes - 1 - second_new
                codes_table[code_index, first_axis * edge_nodes + second_axis] = first_new * edge_nodes + second_new
    return codes_table

def condense(coeffs, element_loads, basis_mats):
    element_mats = jnp.einsum('ek,kab->eab', coeffs, basis_mats, precision=full_precision)
    inner_block = element_mats[:, :CELL_DOFS, :CELL_DOFS]
    coupling = element_mats[:, :CELL_DOFS, CELL_DOFS:]
    outer_block = element_mats[:, CELL_DOFS:, CELL_DOFS:]
    factor = jnp.linalg.cholesky(inner_block)
    solved = jax.scipy.linalg.solve_triangular(factor, coupling, lower=True)
    source = jax.scipy.linalg.solve_triangular(factor, element_loads[:, :CELL_DOFS, None], lower=True)[:, :, 0]
    schur_part = outer_block - jnp.einsum('eib,eic->ebc', solved, solved, precision=full_precision)
    load_trace = element_loads[:, CELL_DOFS:] - jnp.einsum('eib,ei->eb', solved, source, precision=full_precision)
    return (schur_part, load_trace)

def reference(basis_mats, coeffs, element_loads, elem_faces, orient_codes, shared_owned, shared_remote, lower_peers, upper_peers):
    devices = N_GX * N_GY
    elem_total = devices * ELEM_DEV
    face_total = devices * FACE_DEV
    grouped = (coeffs.reshape(devices, ELEM_DEV, TERMS), element_loads.reshape(devices, ELEM_DEV, LOCAL_DOFS))
    schur_blocks, load_trace = lax.map(lambda pieces: condense(pieces[0], pieces[1], basis_mats), grouped)
    schur_blocks = schur_blocks.reshape(elem_total, TRACE_DOFS, TRACE_DOFS)
    load_trace = load_trace.reshape(elem_total, TRACE_DOFS)
    device_ids = jnp.arange(devices, dtype=jnp.int32)
    first_owner = upper_peers[:, 0]
    first_targets = first_owner[:, None] * FACE_DEV + shared_owned[first_owner, 0, :]
    remote_map = jnp.zeros((devices, REMOTE), jnp.int32).at[device_ids[:, None], shared_remote[:, 0, :]].set(first_targets)
    second_users = lower_peers[:, 1]
    second_targets = device_ids[:, None] * FACE_DEV + shared_owned[:, 1, :]
    remote_map = remote_map.at[second_users[:, None], shared_remote[second_users, 1, :]].set(second_targets)
    slot_values = elem_faces.reshape(devices, ELEM_DEV * 6)
    remote_pick = jnp.take_along_axis(remote_map, jnp.clip(slot_values - FACE_DEV, 0, REMOTE - 1).astype(jnp.int32), axis=1)
    face_of = jnp.where(slot_values < FACE_DEV, device_ids[:, None] * FACE_DEV + slot_values, remote_pick).reshape(elem_total, 6)
    codes_table = orient_table()
    forward_idx = jnp.asarray(codes_table)[orient_codes]
    backward_idx = jnp.asarray(np.argsort(codes_table, axis=1).astype(np.int32))[orient_codes]

    def spread(field_values):
        gathered = field_values.T[face_of]
        return jnp.take_along_axis(gathered, forward_idx, axis=2).reshape(elem_total, TRACE_DOFS)

    def collect(element_values):
        placed = jnp.take_along_axis(element_values.reshape(elem_total, 6, FACE_DOFS), backward_idx, axis=2)
        summed = jax.ops.segment_sum(placed.reshape(elem_total * 6, FACE_DOFS), face_of.reshape(-1), num_segments=face_total)
        return summed.T

    def operate(field_values):
        return collect(jnp.einsum('ekl,el->ek', schur_blocks, spread(field_values), precision=full_precision))
    rhs_faces = collect(load_trace)
    diag_faces = collect(jnp.diagonal(schur_blocks, axis1=1, axis2=2))
    trace = jnp.zeros_like(rhs_faces)
    residual = rhs_faces
    precond = residual / diag_faces
    direction = precond
    rz_now = jnp.sum(residual * precond)
    for iteration in range(ITERS):
        mapped = operate(direction)
        step_size = rz_now / jnp.sum(direction * mapped)
        trace = trace + step_size * direction
        residual = residual - step_size * mapped
        precond = residual / diag_faces
        rz_next = jnp.sum(residual * precond)
        direction = precond + rz_next / rz_now * direction
        rz_now = rz_next
    return (trace, residual)
```

```python
import jax
import jax.numpy as jnp
import numpy as np
from jax import lax
from jax.experimental import pallas as pl
from jax.experimental.pallas import tpu as pltpu
from jax.sharding import PartitionSpec as P

SIDE = 5
FACE_DOFS = 25
CELL_DOFS = 125
TRACE_DOFS = 150
LOCAL_DOFS = 275
TERMS = 12
ITERS = 4
ELEM_DEV = 16
FACE_DEV = 64
SHARED = 4
REMOTE = 8
SLOTS = FACE_DEV + REMOTE
ROWS = 6 * ELEM_DEV
PIVOT = 16
CELL_PAD = 128
TRACE_PAD = 152
LOAD_LANE = TRACE_DOFS
WIDE = 256

INTERPRET = False
f32 = jnp.float32
full_precision = lax.Precision.HIGHEST


def mm(a, b):
    return jnp.dot(a, b, precision=full_precision, preferred_element_type=f32)


def mm_ta(a, b):
    return lax.dot_general(
        a, b, (((0,), (0,)), ((), ())), precision=full_precision, preferred_element_type=f32
    )


def orient_table():
    n = SIDE
    table = np.zeros((8, n * n), np.int32)
    for code in range(8):
        for a in range(n):
            for b in range(n):
                a2, b2 = (b, a) if code & 1 else (a, b)
                if code & 2:
                    a2 = n - 1 - a2
                if code & 4:
                    b2 = n - 1 - b2
                table[code, a * n + b] = a2 * n + b2
    return table


def place_matrix():
    table = orient_table()
    place = np.zeros((WIDE, WIDE), np.float32)
    for code in range(8):
        for q in range(FACE_DOFS):
            for j in range(6):
                place[code * 32 + table[code, q], j * FACE_DOFS + q] = 1.0
    return place


def iota(shape, axis):
    return lax.broadcasted_iota(jnp.int32, shape, axis)


def retile(x):
    x = x + pltpu.roll(x, 64, 1)
    return x + pltpu.roll(x, 32, 1)


def code_mask(codes):
    return iota((ROWS, WIDE), 1) // 32 == codes


def spread(field, slots_col, codes_col, place):
    pick = (iota((ROWS, SLOTS), 1) == slots_col).astype(f32)
    rows = mm(pick, field)
    rows = jnp.concatenate([rows, rows], axis=1)
    lanes = iota((ROWS, WIDE), 1)
    valid = (lanes // 32 == codes_col) & (lanes % 32 < FACE_DOFS)
    rows = jnp.where(valid, rows, 0.0)
    placed = mm(rows, place)
    lane = iota((ELEM_DEV, WIDE), 1)
    total = jnp.zeros((ELEM_DEV, WIDE), f32)
    for j in range(6):
        mine = (lane >= j * FACE_DOFS) & (lane < (j + 1) * FACE_DOFS)
        total = total + jnp.where(mine, placed[j * ELEM_DEV : (j + 1) * ELEM_DEV], 0.0)
    return total


def collect(values, slots_row, codes_col, place_t):
    lane = iota((ELEM_DEV, WIDE), 1)
    parts = []
    for j in range(6):
        mine = (lane >= j * FACE_DOFS) & (lane < (j + 1) * FACE_DOFS)
        parts.append(jnp.where(mine, values, 0.0))
    turned = mm(jnp.concatenate(parts, axis=0), place_t)
    turned = jnp.where(code_mask(codes_col), turned, 0.0)
    pick_t = (iota((SLOTS, ROWS), 0) == slots_row).astype(f32)
    summed = mm(pick_t, turned)
    return retile(summed[:, :128] + summed[:, 128:])


def message(ref, lists_ref, m):
    block = iota((1, 128), 1) // 32
    row = ref[pl.ds(lists_ref[m, 0], 1), :]
    for k in range(1, SHARED):
        row = jnp.where(block == k, ref[pl.ds(lists_ref[m, k], 1), :], row)
    return jnp.where(iota((1, 128), 1) % 32 < FACE_DOFS, row, 0.0)


def settle(ref, incoming, lists_ref):
    block = iota((1, 128), 1) // 32
    inside = iota((1, 128), 1) % 32 < FACE_DOFS
    rows = []
    for m in range(4):
        row = jnp.where(inside, incoming[m], 0.0)
        for k in range(SHARED):
            rows.append(jnp.where(block == k, row, 0.0))
    rows = retile(jnp.concatenate(rows, axis=0))
    for m in range(4):
        for k in range(SHARED):
            at = pl.ds(lists_ref[m, k], 1)
            ref[at, :] = ref[at, :] + rows[m * SHARED + k : m * SHARED + k + 1]


def row_tile(row):
    return pl.ds(pl.multiple_of(row // 8 * 8, 8), 8), iota((8, 128), 0) == row % 8


def write_bucket(out_ref, fill, peers_ref, rows, fields):
    span = 128 * fields
    out_ref[...] = fill
    for m in range(4):
        at, hit = row_tile(peers_ref[m])
        start = span * (m // 2)
        for n in range(fields):
            cut = slice(start + 128 * n, start + 128 * (n + 1))
            out_ref[at, cut] = out_ref[at, cut] + jnp.where(hit, rows[m][n], 0.0)


def read_bucket(in_ref, peers_ref, fields, n):
    span = 128 * fields
    got = []
    for m in range(4):
        start = span * (1 - m // 2) + 128 * n
        at, hit = row_tile(peers_ref[m])
        tile = jnp.where(hit, in_ref[at, start : start + 128], 0.0)
        got.append(jnp.sum(tile, axis=0, keepdims=True))
    return got


def invert_blocks(x):
    n = PIVOT
    halves = n // 8
    sub = iota((8, 128), 0)
    for k in range(n):
        kh, ks = k // 8, k % 8
        hit = sub == ks
        factors = [jnp.broadcast_to(x[i][kh][ks : ks + 1], (8, 128)) for i in range(n)]
        inv = 1.0 / factors[k]
        lead = [x[k][h] * inv for h in range(halves)]
        lead[kh] = jnp.where(hit, inv, lead[kh])
        for i in range(n):
            if i == k:
                continue
            for h in range(halves):
                old = jnp.where(hit, 0.0, x[i][h]) if h == kh else x[i][h]
                x[i][h] = old - factors[i] * lead[h]
        x[k] = lead
    return x


def condense_kernel(
    coeffs_ref,
    peers_ref,
    lists_ref,
    basis_ref,
    load_rows_ref,
    load_cols_ref,
    slots_row_ref,
    cols_ref,
    place_t_ref,
    schur_ref,
    fields_ref,
    bucket_ref,
    shifted_ref,
    panel_ref,
    scaled_ref,
    inverse_ref,
    diag_ref,
    load_ref,
):
    width = CELL_PAD + WIDE

    def shift(k, carry):
        shifted_ref[k, 0:128, 0:125] = basis_ref[k, 0:128, 0:125]
        shifted_ref[k, 0:128, 125:128] = jnp.zeros((128, 3), f32)
        shifted_ref[k, 0:128, 128:278] = basis_ref[k, 0:128, 125:275]
        shifted_ref[k, 0:128, 278:384] = jnp.zeros((128, 106), f32)
        shifted_ref[k, 128:278, 128:278] = basis_ref[k, 125:275, 125:275]
        shifted_ref[k, 128:280, 278:384] = jnp.zeros((152, 106), f32)
        return carry

    lax.fori_loop(0, TERMS, shift, 0)

    def cell_rows(g, carry):
        at = pl.ds(pl.multiple_of(g * 8, 8), 8)
        terms = [shifted_ref[k, at, :] for k in range(TERMS)]
        for e in range(ELEM_DEV):
            total = coeffs_ref[e, 0] * terms[0]
            for k in range(1, TERMS):
                total = total + coeffs_ref[e, k] * terms[k]
            panel_ref[e, at, :] = total
        return carry

    lax.fori_loop(0, CELL_PAD // 8, cell_rows, 0)

    def trace_rows(g, carry):
        at = pl.ds(pl.multiple_of(g * 8, 8), 8)
        source = pl.ds(pl.multiple_of(CELL_PAD + g * 8, 8), 8)
        terms = [shifted_ref[k, source, CELL_PAD:] for k in range(TERMS)]
        for e in range(ELEM_DEV):
            total = coeffs_ref[e, 0] * terms[0]
            for k in range(1, TERMS):
                total = total + coeffs_ref[e, k] * terms[k]
            schur_ref[e, at, :] = total
        return carry

    lax.fori_loop(0, TRACE_PAD // 8, trace_rows, 0)

    unit = (iota((3, width), 1) == iota((3, width), 0) + CELL_DOFS).astype(f32)
    load_lane = iota((CELL_PAD, 128), 1) == (CELL_PAD + LOAD_LANE) % 128
    for e in range(ELEM_DEV):
        panel_ref[e, CELL_DOFS:CELL_PAD, :] = unit
        column = jnp.broadcast_to(load_cols_ref[:, e : e + 1], (CELL_PAD, 128))
        panel_ref[e, :, 256:384] = jnp.where(load_lane, column, panel_ref[e, :, 256:384])
        schur_ref[e, LOAD_LANE : LOAD_LANE + 1, :] = load_rows_ref[e : e + 1, :]
        schur_ref[e, LOAD_LANE + 1 : TRACE_PAD, :] = jnp.zeros((1, WIDE), f32)

    group = iota((ELEM_DEV, 128), 1) // PIVOT
    for step in range(CELL_PAD // PIVOT):
        base = step * PIVOT
        own = slice(base, base + PIVOT)
        if step > 0:
            for e in range(ELEM_DEV):
                left = panel_ref[e, 0:base, own]
                panel_ref[e, own, :] = panel_ref[e, own, :] - mm_ta(left, scaled_ref[e, 0:base, :])
        x = []
        for half in range(PIVOT // 8):
            packed = jnp.zeros((ELEM_DEV, 128), f32)
            for s in range(8):
                slab = panel_ref[:, base + half * 8 + s, 0:128]
                turn = (s * PIVOT - base) % 128
                if turn:
                    slab = pltpu.roll(slab, turn, 1)
                packed = jnp.where(group == s, slab, packed)
            tall = jnp.concatenate([packed, jnp.zeros((128 - ELEM_DEV, 128), f32)], axis=0).T
            for s in range(8):
                x.append([tall[s * PIVOT + 8 * h : s * PIVOT + 8 * h + 8] for h in range(PIVOT // 8)])
        x = invert_blocks(x)
        for half in range(PIVOT // 8):
            tall = jnp.concatenate([v for s in range(8) for v in x[half * 8 + s]], axis=0)
            packed = tall.T[:ELEM_DEV]
            for s in range(8):
                turned = pltpu.roll(packed, (-s * PIVOT) % 128, 1) if s else packed
                inverse_ref[:, half * 8 + s, :] = turned
        for e in range(ELEM_DEV):
            scaled_ref[e, own, :] = mm(inverse_ref[e, :, 0:PIVOT], panel_ref[e, own, :])

    diagonal = iota((TRACE_PAD, WIDE), 0) == iota((TRACE_PAD, WIDE), 1)
    for e in range(ELEM_DEV):
        left = panel_ref[e, :, CELL_PAD : CELL_PAD + WIDE]
        block = schur_ref[e] - mm_ta(left, scaled_ref[e, :, CELL_PAD : CELL_PAD + WIDE])[:TRACE_PAD]
        schur_ref[e] = block
        diag_ref[e : e + 1, :] = jnp.sum(jnp.where(diagonal, block, 0.0), axis=0, keepdims=True)
        load_ref[e : e + 1, :] = block[LOAD_LANE : LOAD_LANE + 1]

    codes = cols_ref[:, 1:2]
    fields_ref[0] = collect(load_ref[...], slots_row_ref[...], codes, place_t_ref[...])
    fields_ref[1] = collect(diag_ref[...], slots_row_ref[...], codes, place_t_ref[...])
    rows = [[message(fields_ref.at[n], lists_ref, m) for n in range(2)] for m in range(4)]
    write_bucket(bucket_ref, jnp.zeros(bucket_ref.shape, f32), peers_ref, rows, 2)


def sum_rows(x):
    total = x[0:8]
    for at in range(8, x.shape[0], 8):
        total = total + x[at : at + 8]
    return jnp.sum(total, axis=0, keepdims=True)


def total_of(x):
    return jnp.sum(jnp.sum(x, axis=0, keepdims=True), axis=1, keepdims=True)


def apply_and_send(
    r, z, q, schur_ref, slots_row_ref, cols_ref, place_ref, place_t_ref, peers_ref, lists_ref,
    partial_ref, bucket_ref, image_ref,
):
    codes = cols_ref[:, 1:2]
    x = spread(z, cols_ref[:, 0:1], codes, place_ref[...])
    xt = jnp.concatenate([x[:, 0:128], jnp.zeros((112, 128), f32)], axis=0).T
    xt2 = jnp.concatenate([x[:, 128:256], jnp.zeros((112, 128), f32)], axis=0).T[: TRACE_PAD - 128]
    xt = jnp.concatenate([xt, xt2], axis=0)
    for e in range(ELEM_DEV):
        column = xt[:, e : e + 1]
        image_ref[e : e + 1, :] = jnp.sum(schur_ref[e] * column, axis=0, keepdims=True)
    images = image_ref[...]
    quad = total_of(x * images)
    own = (iota((FACE_DEV, 128), 1) < FACE_DOFS)
    rz = total_of(jnp.where(own, r[:FACE_DEV] * z[:FACE_DEV], 0.0))
    zq = total_of(jnp.where(own, z[:FACE_DEV] * q[:FACE_DEV], 0.0))
    partial_ref[...] = collect(images, slots_row_ref[...], codes, place_t_ref[...])
    rows = [[message(partial_ref, lists_ref, m)] for m in range(4)]
    lane = iota((1, bucket_ref.shape[1]), 1)
    sums = jnp.where(lane == 25, quad, jnp.where(lane == 26, rz, jnp.where(lane == 27, zq, 0.0)))
    write_bucket(bucket_ref, jnp.broadcast_to(sums, bucket_ref.shape), peers_ref, rows, 1)


def start_kernel(
    peers_ref, lists_ref, fields_in_ref, arrived_ref, schur_ref, slots_row_ref, cols_ref, place_ref, place_t_ref,
    state_ref, partial_ref, bucket_ref, fields_ref, image_ref,
):
    fields_ref[...] = fields_in_ref[...]
    for n in range(2):
        settle(fields_ref.at[n], read_bucket(arrived_ref, peers_ref, 2, n), lists_ref)
    inside = iota((SLOTS, 128), 1) % 32 < FACE_DOFS
    r = jnp.where(inside, fields_ref[0], 0.0)
    diag = jnp.where(inside, fields_ref[1], 1.0)
    zero = jnp.zeros((SLOTS, 128), f32)
    z = r / diag
    state_ref[0] = zero
    state_ref[1] = z
    state_ref[2] = r
    state_ref[3] = zero
    state_ref[4] = diag
    state_ref[5] = zero
    apply_and_send(
        r, z, zero, schur_ref, slots_row_ref, cols_ref, place_ref, place_t_ref, peers_ref, lists_ref,
        partial_ref, bucket_ref, image_ref,
    )


def advance(first, peers_ref, lists_ref, partial_in_ref, arrived_ref, state_ref, work_ref):
    work_ref[...] = partial_in_ref[...]
    settle(work_ref, read_bucket(arrived_ref, peers_ref, 1, 0), lists_ref)
    sums = sum_rows(arrived_ref[:, 0:128])
    quad, rz, zq = sums[:, 25:26], sums[:, 26:27], sums[:, 27:28]
    z = state_ref[2] / state_ref[4]
    w = work_ref[...]
    if first:
        direction, image, energy = z, w, quad
    else:
        old_rz, old_energy = state_ref[5, 0:1, 0:1], state_ref[5, 1:2, 0:1]
        beta = rz / old_rz
        direction = z + beta * state_ref[1]
        image = w + beta * state_ref[3]
        energy = quad + 2.0 * beta * zq + beta * beta * old_energy
    alpha = rz / energy
    trace = state_ref[0] + alpha * direction
    residual = state_ref[2] - alpha * image
    return trace, direction, residual, image, rz, energy


def step_kernel(
    first, peers_ref, lists_ref, partial_in_ref, arrived_ref, state_in_ref, schur_ref, slots_row_ref, cols_ref,
    place_ref, place_t_ref, state_ref, partial_ref, bucket_ref, work_ref, image_ref,
):
    trace, direction, residual, image, rz, energy = advance(
        first, peers_ref, lists_ref, partial_in_ref, arrived_ref, state_in_ref, work_ref
    )
    diag = state_in_ref[4]
    state_ref[0] = trace
    state_ref[1] = direction
    state_ref[2] = residual
    state_ref[3] = image
    state_ref[4] = diag
    state_ref[5] = jnp.where(iota((SLOTS, 128), 0) == 0, rz, energy)
    apply_and_send(
        residual, residual / diag, image, schur_ref, slots_row_ref, cols_ref, place_ref, place_t_ref,
        peers_ref, lists_ref, partial_ref, bucket_ref, image_ref,
    )


def finish_kernel(peers_ref, lists_ref, partial_in_ref, arrived_ref, state_in_ref, trace_ref, residual_ref, work_ref):
    trace, _, residual, _, _, _ = advance(
        False, peers_ref, lists_ref, partial_in_ref, arrived_ref, state_in_ref, work_ref
    )
    pad = jnp.zeros((128 - FACE_DEV, 128), f32)
    trace_ref[...] = jnp.concatenate([trace[:FACE_DEV], pad], axis=0).T[:FACE_DOFS, :FACE_DEV]
    residual_ref[...] = jnp.concatenate([residual[:FACE_DEV], pad], axis=0).T[:FACE_DOFS, :FACE_DEV]


VMEM = pl.BlockSpec(memory_space=pltpu.VMEM)
SMEM = pl.BlockSpec(memory_space=pltpu.SMEM)


def shape(*dims):
    return jax.ShapeDtypeStruct(dims, f32)


def call(body, name, scalars, arrays, outs, scratch):
    return pl.pallas_call(
        body,
        name=name,
        in_specs=[SMEM] * len(scalars) + [VMEM] * len(arrays),
        out_specs=[VMEM] * len(outs),
        out_shape=outs,
        scratch_shapes=[pltpu.VMEM(dims, f32) for dims in scratch],
        interpret=INTERPRET,
    )(*scalars, *arrays)


def on_device(
    basis_mats,
    coeffs,
    element_loads,
    elem_faces,
    orient_codes,
    shared_owned,
    shared_remote,
    lower_peers,
    upper_peers,
):
    axes = ("gx", "gy")
    devices = lax.axis_size("gx") * lax.axis_size("gy")
    peers = jnp.concatenate([lower_peers[0], upper_peers[0]])
    lists = jnp.concatenate([shared_owned[0], FACE_DEV + shared_remote[0]], axis=0)
    slots = elem_faces.T.reshape(ROWS)
    codes = orient_codes.T.reshape(ROWS)
    slots_row = slots[None, :]
    cols = jnp.stack([slots, codes], axis=1)
    load_rows = jnp.pad(element_loads[:, CELL_DOFS:], ((0, 0), (0, WIDE - TRACE_DOFS)))
    load_cols = jnp.pad(element_loads[:, :CELL_DOFS].T, ((0, CELL_PAD - CELL_DOFS), (0, 0)))
    place_np = place_matrix()
    place, place_t = jnp.asarray(place_np), jnp.asarray(np.ascontiguousarray(place_np.T))
    width = CELL_PAD + WIDE
    lanes = 256

    def exchange(bucket):
        return lax.all_to_all(bucket, axes, split_axis=0, concat_axis=0, tiled=True)

    schur, fields, bucket = call(
        condense_kernel,
        "condense",
        (coeffs, peers, lists),
        (basis_mats, load_rows, load_cols, slots_row, cols, place_t),
        (shape(ELEM_DEV, TRACE_PAD, WIDE), shape(2, SLOTS, 128), shape(devices, 2 * lanes)),
        (
            (TERMS, CELL_PAD + TRACE_PAD, width),
            (ELEM_DEV, CELL_PAD, width),
            (ELEM_DEV, CELL_PAD, width),
            (ELEM_DEV, PIVOT, 128),
            (ELEM_DEV, WIDE),
            (ELEM_DEV, WIDE),
        ),
    )
    arrived = exchange(bucket)
    state_shapes = (shape(6, SLOTS, 128), shape(SLOTS, 128), shape(devices, lanes))
    fixed = (schur, slots_row, cols, place, place_t)
    state, partial_value, bucket = call(
        start_kernel,
        "start",
        (peers, lists),
        (fields, arrived) + fixed,
        state_shapes,
        ((2, SLOTS, 128), (ELEM_DEV, WIDE)),
    )
    for iteration in range(ITERS - 1):

        def body(*refs, first=iteration == 0):
            step_kernel(first, *refs)

        arrived = exchange(bucket)
        state, partial_value, bucket = call(
            body,
            "step",
            (peers, lists),
            (partial_value, arrived, state) + fixed,
            state_shapes,
            ((SLOTS, 128), (ELEM_DEV, WIDE)),
        )
    arrived = exchange(bucket)
    return tuple(
        call(
            finish_kernel,
            "finish",
            (peers, lists),
            (partial_value, arrived, state),
            (shape(FACE_DOFS, FACE_DEV), shape(FACE_DOFS, FACE_DEV)),
            ((SLOTS, 128),),
        )
    )


def solution(mesh):
    placed = (
        P(),
        P(("gx", "gy"), None),
        P(("gx", "gy"), None),
        P(("gx", "gy"), None),
        P(("gx", "gy"), None),
        P(("gx", "gy"), None, None),
        P(("gx", "gy"), None, None),
        P(("gx", "gy"), None),
        P(("gx", "gy"), None),
    )
    return jax.shard_map(
        on_device,
        mesh=mesh,
        in_specs=placed,
        out_specs=(P(None, ("gx", "gy")), P(None, ("gx", "gy"))),
        check_vma=False,
    )
```

```python
import jax
import jax.numpy as jnp
import numpy as np
from jax import lax
from jax.experimental import pallas as pl
from jax.experimental.pallas import tpu as pltpu
from jax.sharding import PartitionSpec as P

SIDE = 5
FACE_DOFS = 25
CELL_DOFS = 125
TRACE_DOFS = 150
LOCAL_DOFS = 275
TERMS = 12
ITERS = 4
ELEM_DEV = 16
FACE_DEV = 64
SHARED = 4
REMOTE = 8
SLOTS = FACE_DEV + REMOTE
ROWS = 6 * ELEM_DEV
PIVOT = 16
CELL_PAD = 128
TRACE_PAD = 152
LOAD_LANE = TRACE_DOFS
WIDE = 256

INTERPRET = False
f32 = jnp.float32
bf16 = jnp.bfloat16
full_precision = lax.Precision.HIGHEST


def mm(a, b):
    return jnp.dot(a, b, precision=full_precision, preferred_element_type=f32)


def mm_ta(a, b):
    return lax.dot_general(
        a, b, (((0,), (0,)), ((), ())), precision=full_precision, preferred_element_type=f32
    )


def thirds(x):
    high = x.astype(bf16)
    rest = x - high.astype(f32)
    middle = rest.astype(bf16)
    return high, middle, (rest - middle.astype(f32)).astype(bf16)


def pick_left(mask, x):
    return sum(jnp.dot(mask, part, preferred_element_type=f32) for part in thirds(x))


def pick_right(x, mask, contract=0):
    dims = (((1,), (contract,)), ((), ()))
    return sum(lax.dot_general(part, mask, dims, preferred_element_type=f32) for part in thirds(x))


def orient_table():
    n = SIDE
    table = np.zeros((8, n * n), np.int32)
    for code in range(8):
        for a in range(n):
            for b in range(n):
                a2, b2 = (b, a) if code & 1 else (a, b)
                if code & 2:
                    a2 = n - 1 - a2
                if code & 4:
                    b2 = n - 1 - b2
                table[code, a * n + b] = a2 * n + b2
    return table


def place_matrix():
    table = orient_table()
    place = np.zeros((WIDE, WIDE), np.float32)
    for code in range(8):
        for q in range(FACE_DOFS):
            for j in range(6):
                place[code * 32 + table[code, q], j * FACE_DOFS + q] = 1.0
    return place


def iota(shape, axis):
    return lax.broadcasted_iota(jnp.int32, shape, axis)


def retile(x):
    x = x + pltpu.roll(x, 64, 1)
    return x + pltpu.roll(x, 32, 1)


def spread(field, pick, valid, place):
    rows = pick_left(pick, field)
    rows = jnp.concatenate([rows, rows], axis=1) * valid
    placed = pick_right(rows, place)
    lane = iota((ELEM_DEV, WIDE), 1)
    total = jnp.zeros((ELEM_DEV, WIDE), f32)
    for j in range(6):
        mine = (lane >= j * FACE_DOFS) & (lane < (j + 1) * FACE_DOFS)
        total = jnp.where(mine, placed[j * ELEM_DEV : (j + 1) * ELEM_DEV], total)
    return total


def collect(values, pick_t, valid, place):
    lane = iota((ELEM_DEV, WIDE), 1)
    parts = []
    for j in range(6):
        mine = (lane >= j * FACE_DOFS) & (lane < (j + 1) * FACE_DOFS)
        parts.append(jnp.where(mine, values, 0.0))
    turned = pick_right(jnp.concatenate(parts, axis=0), place, 1) * valid
    summed = pick_left(pick_t, turned)
    return retile(summed[:, :128] + summed[:, 128:])


class Links:
    def __init__(self, owned_ref, remote_ref, lower_ref, upper_ref):
        self.owned, self.remote, self.lower, self.upper = owned_ref, remote_ref, lower_ref, upper_ref

    def peer(self, m):
        return (self.lower if m < 2 else self.upper)[0, m % 2]

    def slot(self, m, k):
        if m < 2:
            return self.owned[0, m, k]
        return FACE_DEV + self.remote[0, m - 2, k]

    def clash(self):
        hits = [jnp.where(self.peer(i) == self.peer(2 + j), 1, 0) for i in range(2) for j in range(2)]
        return jnp.where(hits[0] + hits[1] + hits[2] + hits[3] > 0, 1.0, 0.0)


def message(ref, links, m):
    block = iota((1, 128), 1) // 32
    row = ref[pl.ds(links.slot(m, 0), 1), :]
    for k in range(1, SHARED):
        row = jnp.where(block == k, ref[pl.ds(links.slot(m, k), 1), :], row)
    return row


def settle(ref, incoming, links):
    block = iota((1, 128), 1) // 32
    inside = iota((1, 128), 1) % 32 < FACE_DOFS
    rows = []
    for m in range(4):
        row = jnp.where(inside, incoming[m], 0.0)
        for k in range(SHARED):
            rows.append(jnp.where(block == k, row, 0.0))
    rows = retile(jnp.concatenate(rows, axis=0))
    for m in range(4):
        for k in range(SHARED):
            at = pl.ds(links.slot(m, k), 1)
            ref[at, :] = ref[at, :] + rows[m * SHARED + k : m * SHARED + k + 1]


def write_bucket(out_ref, fill, links, rows, wide):
    count = len(rows[0])
    out_ref[...] = jnp.broadcast_to(fill, out_ref.shape)
    keep = iota((1, 128), 1) % 32 < FACE_DOFS
    for m in range(4):
        start = links.peer(m) * (2 * count if wide else count) + (count * (m // 2) if wide else 0)
        for n in range(count):
            out_ref[pl.ds(start + n, 1), :] = jnp.where(keep, rows[m][n], fill)


def read_bucket(in_ref, links, count, n, wide):
    got = []
    for m in range(4):
        start = links.peer(m) * (2 * count if wide else count) + (count * (1 - m // 2) if wide else 0)
        got.append(in_ref[pl.ds(start + n, 1), :])
    return got


def invert_blocks(x):
    n = PIVOT
    halves = n // 8
    sub = iota((8, 128), 0)
    for k in range(n):
        kh, ks = k // 8, k % 8
        hit = sub == ks
        factors = [jnp.broadcast_to(x[i][kh][ks : ks + 1], (8, 128)) for i in range(n)]
        inv = 1.0 / factors[k]
        lead = [x[k][h] * inv for h in range(halves)]
        lead[kh] = jnp.where(hit, inv, lead[kh])
        for i in range(n):
            if i == k:
                continue
            for h in range(halves):
                old = jnp.where(hit, 0.0, x[i][h]) if h == kh else x[i][h]
                x[i][h] = old - factors[i] * lead[h]
        x[k] = lead
    return x


def condense_kernel(
    coeffs_ref,
    owned_ref,
    remote_ref,
    lower_ref,
    upper_ref,
    basis_ref,
    loads_ref,
    faces_ref,
    codes_ref,
    place_ref,
    schur_ref,
    fields_ref,
    pick_ref,
    pick_t_ref,
    valid_ref,
    bucket_ref,
    shifted_ref,
    panel_ref,
    scaled_ref,
    inverse_ref,
    diag_ref,
    load_ref,
    terms_ref,
    copies,
):
    links = Links(owned_ref, remote_ref, lower_ref, upper_ref)
    width = CELL_PAD + WIDE

    def copy_in(k):
        return pltpu.make_async_copy(basis_ref.at[k], terms_ref.at[k], copies.at[k])

    for k in range(TERMS):
        copy_in(k).start()

    def shift(k, carry):
        copy_in(k).wait()
        shifted_ref[k, 0:128, 0:125] = terms_ref[k, 0:128, 0:125]
        shifted_ref[k, 0:128, 125:128] = jnp.zeros((128, 3), f32)
        shifted_ref[k, 0:128, 128:278] = terms_ref[k, 0:128, 125:275]
        shifted_ref[k, 0:128, 278:384] = jnp.zeros((128, 106), f32)
        shifted_ref[k, 128:278, 128:278] = terms_ref[k, 125:275, 125:275]
        shifted_ref[k, 128:280, 278:384] = jnp.zeros((152, 106), f32)
        return carry

    lax.fori_loop(0, TERMS, shift, 0)

    def cell_rows(g, carry):
        at = pl.ds(pl.multiple_of(g * 8, 8), 8)
        terms = [shifted_ref[k, at, :] for k in range(TERMS)]
        for e in range(ELEM_DEV):
            total = coeffs_ref[e, 0] * terms[0]
            for k in range(1, TERMS):
                total = total + coeffs_ref[e, k] * terms[k]
            panel_ref[e, at, :] = total
        return carry

    lax.fori_loop(0, CELL_PAD // 8, cell_rows, 0)

    def trace_rows(g, carry):
        at = pl.ds(pl.multiple_of(g * 8, 8), 8)
        source = pl.ds(pl.multiple_of(CELL_PAD + g * 8, 8), 8)
        terms = [shifted_ref[k, source, CELL_PAD:] for k in range(TERMS)]
        for e in range(ELEM_DEV):
            total = coeffs_ref[e, 0] * terms[0]
            for k in range(1, TERMS):
                total = total + coeffs_ref[e, k] * terms[k]
            schur_ref[e, at, :] = total
        return carry

    lax.fori_loop(0, TRACE_PAD // 8, trace_rows, 0)

    unit = (iota((3, width), 1) == iota((3, width), 0) + CELL_DOFS).astype(f32)
    load_lane = iota((CELL_PAD, 128), 1) == (CELL_PAD + LOAD_LANE) % 128
    pad = jnp.zeros((128 - ELEM_DEV, 128), f32)
    load_cols = jnp.concatenate([loads_ref[:, 0:128], pad], axis=0).T
    for e in range(ELEM_DEV):
        column = jnp.broadcast_to(load_cols[:, e : e + 1], (CELL_PAD, 128))
        panel_ref[e, :, 256:384] = jnp.where(load_lane, column, panel_ref[e, :, 256:384])
        panel_ref[e, CELL_DOFS:CELL_PAD, :] = unit
        schur_ref[e, LOAD_LANE:TRACE_PAD, :] = jnp.zeros((TRACE_PAD - LOAD_LANE, WIDE), f32)
        schur_ref[e, LOAD_LANE : LOAD_LANE + 1, 0:TRACE_DOFS] = loads_ref[e : e + 1, CELL_DOFS:LOCAL_DOFS]

    group = iota((ELEM_DEV, 128), 1) // PIVOT
    for step in range(CELL_PAD // PIVOT):
        base = step * PIVOT
        own = slice(base, base + PIVOT)
        if step > 0:
            for e in range(ELEM_DEV):
                left = panel_ref[e, 0:base, own]
                panel_ref[e, own, :] = panel_ref[e, own, :] - mm_ta(left, scaled_ref[e, 0:base, :])
        x = []
        for half in range(PIVOT // 8):
            packed = jnp.zeros((ELEM_DEV, 128), f32)
            for s in range(8):
                slab = panel_ref[:, base + half * 8 + s, 0:128]
                turn = (s * PIVOT - base) % 128
                if turn:
                    slab = pltpu.roll(slab, turn, 1)
                packed = jnp.where(group == s, slab, packed)
            tall = jnp.concatenate([packed, jnp.zeros((128 - ELEM_DEV, 128), f32)], axis=0).T
            for s in range(8):
                x.append([tall[s * PIVOT + 8 * h : s * PIVOT + 8 * h + 8] for h in range(PIVOT // 8)])
        x = invert_blocks(x)
        for half in range(PIVOT // 8):
            tall = jnp.concatenate([v for s in range(8) for v in x[half * 8 + s]], axis=0)
            packed = tall.T[:ELEM_DEV]
            for s in range(8):
                turned = pltpu.roll(packed, (-s * PIVOT) % 128, 1) if s else packed
                inverse_ref[:, half * 8 + s, :] = turned
        for e in range(ELEM_DEV):
            scaled_ref[e, own, :] = mm(inverse_ref[e, :, 0:PIVOT], panel_ref[e, own, :])

    diagonal = iota((TRACE_PAD, WIDE), 0) == iota((TRACE_PAD, WIDE), 1)

    def finish(e, carry):
        left = panel_ref[e, :, CELL_PAD : CELL_PAD + WIDE]
        block = schur_ref[e] - mm_ta(left, scaled_ref[e, :, CELL_PAD : CELL_PAD + WIDE])[:TRACE_PAD]
        schur_ref[e] = block
        at = pl.ds(e, 1)
        diag_ref[at] = jnp.sum(jnp.where(diagonal, block, 0.0), axis=0, keepdims=True)[None]
        load_ref[at] = block[LOAD_LANE : LOAD_LANE + 1][None]
        return carry

    lax.fori_loop(0, ELEM_DEV, finish, 0, unroll=4)

    faces_row = faces_ref[...].astype(f32)
    square = jnp.zeros((122, 128), f32)
    fill = jnp.zeros((6, 128 - ELEM_DEV), f32)
    faces_t = jnp.concatenate([jnp.concatenate([faces_row, fill], axis=1), square], axis=0).T
    codes_t = jnp.concatenate([jnp.concatenate([codes_ref[...].astype(f32), fill], axis=1), square], axis=0).T
    slots_col = jnp.concatenate([faces_t[:ELEM_DEV, j : j + 1] for j in range(6)], axis=0)
    codes_col = jnp.concatenate([codes_t[:ELEM_DEV, j : j + 1] for j in range(6)], axis=0)
    slots_row = jnp.concatenate([faces_row[j : j + 1] for j in range(6)], axis=1)
    pick_ref[...] = jnp.where(iota((ROWS, SLOTS), 1).astype(f32) == slots_col, 1.0, 0.0).astype(bf16)
    pick_t_ref[...] = jnp.where(iota((SLOTS, ROWS), 0).astype(f32) == slots_row, 1.0, 0.0).astype(bf16)
    lanes = iota((ROWS, WIDE), 1)
    valid = ((lanes // 32).astype(f32) == codes_col) & (lanes % 32 < FACE_DOFS)
    valid_ref[...] = jnp.where(valid, 1.0, 0.0)

    inside = iota((ELEM_DEV, WIDE), 1) < TRACE_DOFS
    for n, ref in enumerate((load_ref, diag_ref)):
        values = jnp.where(inside, ref[...].reshape(ELEM_DEV, WIDE), 0.0)
        fields_ref[n] = collect(values, pick_t_ref[...], valid_ref[...], place_ref[...])
    send_fields(fields_ref, links, bucket_ref, False)


def send_fields(fields_ref, links, bucket_ref, wide):
    rows = [[message(fields_ref.at[n], links, m) for n in range(2)] for m in range(4)]
    fill = jnp.where(iota((1, 128), 1) == 25, links.clash(), 0.0)
    write_bucket(bucket_ref, fill, links, rows, wide)


def resend_kernel(owned_ref, remote_ref, lower_ref, upper_ref, fields_ref, bucket_ref):
    send_fields(fields_ref, Links(owned_ref, remote_ref, lower_ref, upper_ref), bucket_ref, True)


def sum_rows(x):
    total = x[0:8]
    for at in range(8, x.shape[0], 8):
        total = total + x[at : at + 8]
    return jnp.sum(total, axis=0, keepdims=True)


def total_of(x):
    return jnp.sum(jnp.sum(x, axis=0, keepdims=True), axis=1, keepdims=True)


def apply_and_send(r, z, q, links, fixed, partial_ref, bucket_ref, image_ref, wide):
    schur_ref, pick_ref, pick_t_ref, valid_ref, place_ref = fixed
    x = spread(z, pick_ref[...], valid_ref[...], place_ref[...])
    pad = jnp.zeros((128 - ELEM_DEV, 128), f32)
    head = jnp.concatenate([x[:, 0:128], pad], axis=0).T
    tail = jnp.concatenate([x[:, 128:256], pad], axis=0).T[: TRACE_PAD - 128]
    columns = jnp.concatenate([head, tail], axis=0)
    for e in range(ELEM_DEV):
        image_ref[e : e + 1, :] = jnp.sum(schur_ref[e] * columns[:, e : e + 1], axis=0, keepdims=True)
    images = image_ref[...]
    quad = total_of(x * images)
    own = iota((FACE_DEV, 128), 1) < FACE_DOFS
    rz = total_of(jnp.where(own, r[:FACE_DEV] * z[:FACE_DEV], 0.0))
    zq = total_of(jnp.where(own, z[:FACE_DEV] * q[:FACE_DEV], 0.0))
    partial_ref[...] = collect(images, pick_t_ref[...], valid_ref[...], place_ref[...])
    rows = [[message(partial_ref, links, m)] for m in range(4)]
    lane = iota((1, 128), 1)
    sums = jnp.where(lane == 25, quad, jnp.where(lane == 26, rz, jnp.where(lane == 27, zq, 0.0)))
    write_bucket(bucket_ref, sums, links, rows, wide)


def start_kernel(wide, owned_ref, remote_ref, lower_ref, upper_ref, fields_in_ref, arrived_ref, *refs):
    links = Links(owned_ref, remote_ref, lower_ref, upper_ref)
    fixed, (state_ref, partial_ref, bucket_ref, clash_ref, fields_ref, image_ref) = refs[:5], refs[5:]
    clash_ref[0] = jnp.sum(sum_rows(arrived_ref[...])[:, 25:26])
    fields_ref[...] = fields_in_ref[...]
    for n in range(2):
        settle(fields_ref.at[n], read_bucket(arrived_ref, links, 2, n, wide), links)
    inside = iota((SLOTS, 128), 1) % 32 < FACE_DOFS
    r = jnp.where(inside, fields_ref[0], 0.0)
    diag = jnp.where(inside, fields_ref[1], 1.0)
    zero = jnp.zeros((SLOTS, 128), f32)
    z = r / diag
    state_ref[0] = zero
    state_ref[1] = zero
    state_ref[2] = r
    state_ref[3] = zero
    state_ref[4] = diag
    state_ref[5] = jnp.where(iota((SLOTS, 128), 0) == 0, jnp.inf, 0.0)
    apply_and_send(r, z, zero, links, fixed, partial_ref, bucket_ref, image_ref, wide)


def advance(wide, links, partial_in_ref, arrived_ref, state_ref, work_ref):
    work_ref[...] = partial_in_ref[...]
    settle(work_ref, read_bucket(arrived_ref, links, 1, 0, wide), links)
    sums = sum_rows(arrived_ref[...])
    if wide:
        sums = sums * 0.5
    quad, rz, zq = sums[:, 25:26], sums[:, 26:27], sums[:, 27:28]
    old_rz, old_energy = state_ref[5, 0:1, 0:1], state_ref[5, 1:2, 0:1]
    beta = rz / old_rz
    direction = state_ref[2] / state_ref[4] + beta * state_ref[1]
    image = work_ref[...] + beta * state_ref[3]
    energy = quad + 2.0 * beta * zq + beta * beta * old_energy
    alpha = rz / energy
    trace = state_ref[0] + alpha * direction
    residual = state_ref[2] - alpha * image
    return trace, direction, residual, image, rz, energy


def step_kernel(wide, owned_ref, remote_ref, lower_ref, upper_ref, partial_in_ref, arrived_ref, state_in_ref, *refs):
    links = Links(owned_ref, remote_ref, lower_ref, upper_ref)
    fixed, (state_ref, partial_ref, bucket_ref, work_ref, image_ref) = refs[:5], refs[5:]
    trace, direction, residual, image, rz, energy = advance(
        wide, links, partial_in_ref, arrived_ref, state_in_ref, work_ref
    )
    diag = state_in_ref[4]
    state_ref[0] = trace
    state_ref[1] = direction
    state_ref[2] = residual
    state_ref[3] = image
    state_ref[4] = diag
    state_ref[5] = jnp.where(iota((SLOTS, 128), 0) == 0, rz, energy)
    apply_and_send(
        residual, residual / diag, image, links, fixed, partial_ref, bucket_ref, image_ref, wide
    )


def finish_kernel(
    wide, owned_ref, remote_ref, lower_ref, upper_ref, partial_in_ref, arrived_ref, state_in_ref,
    trace_ref, residual_ref, work_ref,
):
    links = Links(owned_ref, remote_ref, lower_ref, upper_ref)
    trace, _, residual, _, _, _ = advance(wide, links, partial_in_ref, arrived_ref, state_in_ref, work_ref)
    pad = jnp.zeros((128 - FACE_DEV, 128), f32)
    trace_ref[...] = jnp.concatenate([trace[:FACE_DEV], pad], axis=0).T[:FACE_DOFS, :FACE_DEV]
    residual_ref[...] = jnp.concatenate([residual[:FACE_DEV], pad], axis=0).T[:FACE_DOFS, :FACE_DEV]


VMEM = pl.BlockSpec(memory_space=pltpu.VMEM)
SMEM = pl.BlockSpec(memory_space=pltpu.SMEM)
HBM = pl.BlockSpec(memory_space=pl.ANY)


def shape(*dims, dtype=f32):
    return jax.ShapeDtypeStruct(dims, dtype)


def call(body, name, scalars, arrays, outs, scratch, specs=None, out_specs=None):
    return pl.pallas_call(
        body,
        name=name,
        in_specs=[SMEM] * len(scalars) + (specs or [VMEM] * len(arrays)),
        out_specs=out_specs or [VMEM] * len(outs),
        out_shape=outs,
        scratch_shapes=[pltpu.VMEM(item, f32) if isinstance(item, tuple) else item for item in scratch],
        interpret=INTERPRET,
    )(*scalars, *arrays)


def on_device(
    basis_mats,
    coeffs,
    element_loads,
    elem_faces,
    orient_codes,
    shared_owned,
    shared_remote,
    lower_peers,
    upper_peers,
):
    axes = ("gx", "gy")
    devices = lax.axis_size("gx") * lax.axis_size("gy")
    links = (shared_owned, shared_remote, lower_peers, upper_peers)
    place = jnp.asarray(place_matrix(), bf16)
    width = CELL_PAD + WIDE

    def exchange(bucket):
        parts = bucket.shape[0] // devices
        sent = bucket.reshape(devices, parts, 128) if parts > 1 else bucket
        got = lax.all_to_all(sent, axes, split_axis=0, concat_axis=0, tiled=True)
        return got.reshape(bucket.shape)

    schur, fields, pick, pick_t, valid, bucket = call(
        condense_kernel,
        "condense",
        (coeffs,) + links,
        (basis_mats, element_loads, elem_faces.T, orient_codes.T, place),
        (
            shape(ELEM_DEV, TRACE_PAD, WIDE),
            shape(2, SLOTS, 128),
            shape(ROWS, SLOTS, dtype=bf16),
            shape(SLOTS, ROWS, dtype=bf16),
            shape(ROWS, WIDE),
            shape(2 * devices, 128),
        ),
        (
            (TERMS, CELL_PAD + TRACE_PAD, width),
            (ELEM_DEV, CELL_PAD, width),
            (ELEM_DEV, CELL_PAD, width),
            (ELEM_DEV, PIVOT, 128),
            (ELEM_DEV, 1, WIDE),
            (ELEM_DEV, 1, WIDE),
            (TERMS, LOCAL_DOFS, LOCAL_DOFS),
            pltpu.SemaphoreType.DMA((TERMS,)),
        ),
        specs=[HBM] + [VMEM] * 4,
    )
    fixed = (schur, pick, pick_t, valid, place)

    def start(arrived, wide):
        return call(
            lambda *refs: start_kernel(wide, *refs),
            "start_wide" if wide else "start",
            links,
            (fields, arrived) + fixed,
            (shape(6, SLOTS, 128), shape(SLOTS, 128), shape((1 + wide) * devices, 128), shape(1)),
            ((2, SLOTS, 128), (ELEM_DEV, WIDE)),
            out_specs=[VMEM] * 3 + [SMEM],
        )

    def step(state, partial_value, arrived, wide):
        return call(
            lambda *refs: step_kernel(wide, *refs),
            "step_wide" if wide else "step",
            links,
            (partial_value, arrived, state) + fixed,
            (shape(6, SLOTS, 128), shape(SLOTS, 128), shape((1 + wide) * devices, 128)),
            ((SLOTS, 128), (ELEM_DEV, WIDE)),
        )

    def finish(state, partial_value, arrived, wide):
        return tuple(
            call(
                lambda *refs: finish_kernel(wide, *refs),
                "finish_wide" if wide else "finish",
                links,
                (partial_value, arrived, state),
                (shape(FACE_DOFS, FACE_DEV), shape(FACE_DOFS, FACE_DEV)),
                ((SLOTS, 128),),
            )
        )

    def narrow_run(state, partial_value, bucket):
        for _ in range(ITERS - 1):
            state, partial_value, bucket = step(state, partial_value, exchange(bucket), False)
        return finish(state, partial_value, exchange(bucket), False)

    def wide_run(state, partial_value, bucket):
        (again,) = call(resend_kernel, "resend", links, (fields,), (shape(4 * devices, 128),), ())
        state, partial_value, bucket, _ = start(exchange(again), True)

        def body(_, carry):
            state, partial_value, bucket = carry
            return tuple(step(state, partial_value, exchange(bucket), True))

        carry = lax.fori_loop(0, ITERS, body, (state, partial_value, bucket))
        return carry[0][0, :FACE_DEV, :FACE_DOFS].T, carry[0][2, :FACE_DEV, :FACE_DOFS].T

    state, partial_value, bucket, clash = start(exchange(bucket), False)
    return lax.cond(clash[0] > 0.0, wide_run, narrow_run, state, partial_value, bucket)


def solution(mesh):
    placed = (
        P(),
        P(("gx", "gy"), None),
        P(("gx", "gy"), None),
        P(("gx", "gy"), None),
        P(("gx", "gy"), None),
        P(("gx", "gy"), None, None),
        P(("gx", "gy"), None, None),
        P(("gx", "gy"), None),
        P(("gx", "gy"), None),
    )
    return jax.shard_map(
        on_device,
        mesh=mesh,
        in_specs=placed,
        out_specs=(P(None, ("gx", "gy")), P(None, ("gx", "gy"))),
        check_vma=False,
    )
```

```python
import jax
import jax.numpy as jnp
import numpy as np
from jax import lax
from jax.experimental import pallas as pl
from jax.experimental.pallas import tpu as pltpu
from jax.sharding import PartitionSpec as P

SIDE = 5
FACE_DOFS = 25
CELL_DOFS = 125
TRACE_DOFS = 150
LOCAL_DOFS = 275
TERMS = 12
ITERS = 4
ELEM_DEV = 16
FACE_DEV = 64
SHARED = 4
REMOTE = 8
SLOTS = FACE_DEV + REMOTE
ROWS = 6 * ELEM_DEV
PIVOT = 16
CELL_PAD = 128
TRACE_PAD = 152
LOAD_LANE = TRACE_DOFS
WIDE = 256

INTERPRET = False
f32 = jnp.float32
bf16 = jnp.bfloat16


def thirds(x):
    high = x.astype(bf16)
    rest = x - high.astype(f32)
    middle = rest.astype(bf16)
    return high, middle, (rest - middle.astype(f32)).astype(bf16)


def left_parts(parts, axis=0):
    high, middle, low = parts
    return jnp.concatenate([high, high, middle, high, low, middle], axis=axis)


def right_parts(parts):
    high, middle, low = parts
    return jnp.concatenate([high, middle, high, low, high, middle], axis=0)


def product(a, b, contract=0):
    dims = (((contract,), (0,)), ((), ()))
    return lax.dot_general(a, b, dims, preferred_element_type=f32)


def pick_left(mask, x):
    return sum(jnp.dot(mask, part, preferred_element_type=f32) for part in thirds(x))


def pick_right(x, mask, contract=0):
    dims = (((1,), (contract,)), ((), ()))
    return sum(lax.dot_general(part, mask, dims, preferred_element_type=f32) for part in thirds(x))


def orient_table():
    n = SIDE
    table = np.zeros((8, n * n), np.int32)
    for code in range(8):
        for a in range(n):
            for b in range(n):
                a2, b2 = (b, a) if code & 1 else (a, b)
                if code & 2:
                    a2 = n - 1 - a2
                if code & 4:
                    b2 = n - 1 - b2
                table[code, a * n + b] = a2 * n + b2
    return table


def place_matrix():
    table = orient_table()
    place = np.zeros((WIDE, WIDE), np.float32)
    for code in range(8):
        for q in range(FACE_DOFS):
            for j in range(6):
                place[code * 32 + table[code, q], j * FACE_DOFS + q] = 1.0
    return place


def iota(shape, axis):
    return lax.broadcasted_iota(jnp.int32, shape, axis)


def retile(x):
    x = x + pltpu.roll(x, 64, 1)
    return x + pltpu.roll(x, 32, 1)


def spread(field, pick, valid, place):
    rows = pick_left(pick, field)
    rows = jnp.concatenate([rows, rows], axis=1) * valid
    placed = pick_right(rows, place)
    lane = iota((ELEM_DEV, WIDE), 1)
    total = jnp.zeros((ELEM_DEV, WIDE), f32)
    for j in range(6):
        mine = (lane >= j * FACE_DOFS) & (lane < (j + 1) * FACE_DOFS)
        total = jnp.where(mine, placed[j * ELEM_DEV : (j + 1) * ELEM_DEV], total)
    return total


def collect(values, pick_t, valid, place):
    lane = iota((ELEM_DEV, WIDE), 1)
    parts = []
    for j in range(6):
        mine = (lane >= j * FACE_DOFS) & (lane < (j + 1) * FACE_DOFS)
        parts.append(jnp.where(mine, values, 0.0))
    turned = pick_right(jnp.concatenate(parts, axis=0), place, 1) * valid
    summed = pick_left(pick_t, turned)
    return retile(summed[:, :128] + summed[:, 128:])


class Links:
    def __init__(self, owned_ref, remote_ref, lower_ref, upper_ref):
        self.owned, self.remote, self.lower, self.upper = owned_ref, remote_ref, lower_ref, upper_ref

    def peer(self, m):
        return (self.lower if m < 2 else self.upper)[0, m % 2]

    def slot(self, m, k):
        if m < 2:
            return self.owned[0, m, k]
        return FACE_DEV + self.remote[0, m - 2, k]

    def clash(self):
        hits = [jnp.where(self.peer(i) == self.peer(2 + j), 1, 0) for i in range(2) for j in range(2)]
        return jnp.where(hits[0] + hits[1] + hits[2] + hits[3] > 0, 1.0, 0.0)


def message(ref, links, m):
    block = iota((1, 128), 1) // 32
    row = ref[pl.ds(links.slot(m, 0), 1), :]
    for k in range(1, SHARED):
        row = jnp.where(block == k, ref[pl.ds(links.slot(m, k), 1), :], row)
    return row


def settle(ref, incoming, links):
    block = iota((1, 128), 1) // 32
    inside = iota((1, 128), 1) % 32 < FACE_DOFS
    rows = []
    for m in range(4):
        row = jnp.where(inside, incoming[m], 0.0)
        for k in range(SHARED):
            rows.append(jnp.where(block == k, row, 0.0))
    rows = retile(jnp.concatenate(rows, axis=0))
    for m in range(4):
        for k in range(SHARED):
            at = pl.ds(links.slot(m, k), 1)
            ref[at, :] = ref[at, :] + rows[m * SHARED + k : m * SHARED + k + 1]


def write_bucket(out_ref, fill, links, rows, wide):
    count = len(rows[0])
    out_ref[...] = jnp.broadcast_to(fill, out_ref.shape)
    keep = iota((1, 128), 1) % 32 < FACE_DOFS
    for m in range(4):
        start = links.peer(m) * (2 * count if wide else count) + (count * (m // 2) if wide else 0)
        for n in range(count):
            out_ref[pl.ds(start + n, 1), :] = jnp.where(keep, rows[m][n], fill)


def read_bucket(in_ref, links, count, n, wide):
    got = []
    for m in range(4):
        start = links.peer(m) * (2 * count if wide else count) + (count * (1 - m // 2) if wide else 0)
        got.append(in_ref[pl.ds(start + n, 1), :])
    return got


def invert_blocks(x):
    n = PIVOT
    halves = n // 8
    sub = iota((8, 128), 0)
    for k in range(n):
        kh, ks = k // 8, k % 8
        hit = sub == ks
        factors = [jnp.broadcast_to(x[i][kh][ks : ks + 1], (8, 128)) for i in range(n)]
        inv = 1.0 / factors[k]
        lead = [x[k][h] * inv for h in range(halves)]
        lead[kh] = jnp.where(hit, inv, lead[kh])
        for i in range(n):
            if i == k:
                continue
            for h in range(halves):
                old = jnp.where(hit, 0.0, x[i][h]) if h == kh else x[i][h]
                x[i][h] = old - factors[i] * lead[h]
        x[k] = lead
    return x


def condense_kernel(
    coeffs_ref,
    owned_ref,
    remote_ref,
    lower_ref,
    upper_ref,
    basis_ref,
    loads_ref,
    faces_ref,
    codes_ref,
    place_ref,
    schur_ref,
    fields_ref,
    pick_ref,
    pick_t_ref,
    valid_ref,
    bucket_ref,
    shifted_ref,
    panel_ref,
    scaled_ref,
    inverse_ref,
    diag_ref,
    load_ref,
    terms_ref,
    copies,
):
    links = Links(owned_ref, remote_ref, lower_ref, upper_ref)
    width = CELL_PAD + WIDE

    def copy_in(k):
        return pltpu.make_async_copy(basis_ref.at[k], terms_ref.at[k], copies.at[k])

    for k in range(TERMS):
        copy_in(k).start()

    def shift(k, carry):
        copy_in(k).wait()
        shifted_ref[k, 0:128, 0:125] = terms_ref[k, 0:128, 0:125]
        shifted_ref[k, 0:128, 125:128] = jnp.zeros((128, 3), f32)
        shifted_ref[k, 0:128, 128:278] = terms_ref[k, 0:128, 125:275]
        shifted_ref[k, 0:128, 278:384] = jnp.zeros((128, 106), f32)
        shifted_ref[k, 128:278, 128:278] = terms_ref[k, 125:275, 125:275]
        shifted_ref[k, 128:280, 278:384] = jnp.zeros((152, 106), f32)
        return carry

    lax.fori_loop(0, TERMS, shift, 0)

    def cell_rows(g, carry):
        at = pl.ds(pl.multiple_of(g * 8, 8), 8)
        terms = [shifted_ref[k, at, :] for k in range(TERMS)]
        for e in range(ELEM_DEV):
            total = coeffs_ref[e, 0] * terms[0]
            for k in range(1, TERMS):
                total = total + coeffs_ref[e, k] * terms[k]
            panel_ref[e, at, :] = total
        return carry

    lax.fori_loop(0, CELL_PAD // 8, cell_rows, 0)

    def trace_rows(g, carry):
        at = pl.ds(pl.multiple_of(g * 8, 8), 8)
        source = pl.ds(pl.multiple_of(CELL_PAD + g * 8, 8), 8)
        terms = [shifted_ref[k, source, CELL_PAD:] for k in range(TERMS)]
        for e in range(ELEM_DEV):
            total = coeffs_ref[e, 0] * terms[0]
            for k in range(1, TERMS):
                total = total + coeffs_ref[e, k] * terms[k]
            schur_ref[e, at, :] = total
        return carry

    lax.fori_loop(0, TRACE_PAD // 8, trace_rows, 0)

    unit = (iota((3, width), 1) == iota((3, width), 0) + CELL_DOFS).astype(f32)
    load_lane = iota((CELL_PAD, 128), 1) == (CELL_PAD + LOAD_LANE) % 128
    pad = jnp.zeros((128 - ELEM_DEV, 128), f32)
    load_cols = jnp.concatenate([loads_ref[:, 0:128], pad], axis=0).T
    for e in range(ELEM_DEV):
        column = jnp.broadcast_to(load_cols[:, e : e + 1], (CELL_PAD, 128))
        panel_ref[e, :, 256:384] = jnp.where(load_lane, column, panel_ref[e, :, 256:384])
        panel_ref[e, CELL_DOFS:CELL_PAD, :] = unit
        schur_ref[e, LOAD_LANE:TRACE_PAD, :] = jnp.zeros((TRACE_PAD - LOAD_LANE, WIDE), f32)
        schur_ref[e, LOAD_LANE : LOAD_LANE + 1, 0:TRACE_DOFS] = loads_ref[e : e + 1, CELL_DOFS:LOCAL_DOFS]

    group = iota((ELEM_DEV, 128), 1) // PIVOT
    scaled_ref[...] = jnp.zeros(scaled_ref.shape, bf16)

    def folded(x):
        return x[0:PIVOT] + (x[PIVOT : 2 * PIVOT] + x[2 * PIVOT : 3 * PIVOT])

    for step in range(CELL_PAD // PIVOT):
        base = step * PIVOT
        own = slice(base, base + PIVOT)
        if step > 0:
            for e in range(ELEM_DEV):
                depth = 32 if base <= 32 else 64 if base <= 64 else 128
                left = panel_ref[e, 0:base, 0:128].T[own]
                if base < 128:
                    left = jnp.concatenate([left, jnp.zeros((PIVOT, 128 - base), f32)], axis=1)
                if depth == 128:
                    left = jnp.concatenate([left, left, left], axis=1)
                elif depth == 64:
                    left = jnp.concatenate([left + pltpu.roll(left, 64, 1), left], axis=1)
                else:
                    left = left + pltpu.roll(left, 32, 1) + pltpu.roll(left, 64, 1)
                lane = iota(left.shape, 1)
                stacked = jnp.concatenate(
                    [
                        jnp.where(lane < (3 - n) * depth, part.astype(f32), 0.0).astype(bf16)
                        for n, part in enumerate(thirds(left))
                    ],
                    axis=0,
                )[:, 0 : 3 * depth]
                right = jnp.concatenate([scaled_ref[n, e, 0:depth, :] for n in range(3)], axis=0)
                panel_ref[e, own, :] = panel_ref[e, own, :] - folded(product(stacked, right, 1))
        x = []
        for half in range(PIVOT // 8):
            packed = jnp.zeros((ELEM_DEV, 128), f32)
            for s in range(8):
                slab = panel_ref[:, base + half * 8 + s, 0:128]
                turn = (s * PIVOT - base) % 128
                if turn:
                    slab = pltpu.roll(slab, turn, 1)
                packed = jnp.where(group == s, slab, packed)
            tall = jnp.concatenate([packed, jnp.zeros((128 - ELEM_DEV, 128), f32)], axis=0).T
            for s in range(8):
                x.append([tall[s * PIVOT + 8 * h : s * PIVOT + 8 * h + 8] for h in range(PIVOT // 8)])
        x = invert_blocks(x)
        for half in range(PIVOT // 8):
            tall = jnp.concatenate([v for s in range(8) for v in x[half * 8 + s]], axis=0)
            packed = tall.T[:ELEM_DEV]
            for s in range(8):
                first, second, third = (
                    pltpu.roll(packed, (t - s) * PIVOT % 128, 1) if (t - s) % 8 else packed for t in range(3)
                )
                inverse_ref[:, half * 8 + s, :] = jnp.where(group == 0, first, jnp.where(group == 1, second, third))
        for e in range(ELEM_DEV):
            top = panel_ref[e, own, :]
            parts = thirds(inverse_ref[e])
            stacked = jnp.concatenate(
                [
                    jnp.where(group < 3 - n, part.astype(f32), 0.0).astype(bf16)
                    for n, part in enumerate(parts)
                ],
                axis=0,
            )
            right = jnp.concatenate(thirds(top), axis=0)
            scaled = thirds(folded(product(stacked[:, 0 : 3 * PIVOT], right, 1)))
            for n in range(3):
                scaled_ref[n, e, own, :] = scaled[n]

    diagonal = iota((TRACE_PAD, WIDE), 0) == iota((TRACE_PAD, WIDE), 1)

    def finish(e, carry):
        left = panel_ref[e, :, CELL_PAD : CELL_PAD + WIDE].T[:TRACE_PAD]
        right = right_parts([scaled_ref[n, e, :, CELL_PAD : CELL_PAD + WIDE] for n in range(3)])
        block = schur_ref[e] - product(left_parts(thirds(left), 1), right, 1)
        schur_ref[e] = block
        at = pl.ds(e, 1)
        diag_ref[at] = jnp.sum(jnp.where(diagonal, block, 0.0), axis=0, keepdims=True)[None]
        load_ref[at] = block[LOAD_LANE : LOAD_LANE + 1][None]
        return carry

    lax.fori_loop(0, ELEM_DEV, finish, 0, unroll=4)

    faces_row = faces_ref[...].astype(f32)
    square = jnp.zeros((122, 128), f32)
    fill = jnp.zeros((6, 128 - ELEM_DEV), f32)
    faces_t = jnp.concatenate([jnp.concatenate([faces_row, fill], axis=1), square], axis=0).T
    codes_t = jnp.concatenate([jnp.concatenate([codes_ref[...].astype(f32), fill], axis=1), square], axis=0).T
    slots_col = jnp.concatenate([faces_t[:ELEM_DEV, j : j + 1] for j in range(6)], axis=0)
    codes_col = jnp.concatenate([codes_t[:ELEM_DEV, j : j + 1] for j in range(6)], axis=0)
    slots_row = jnp.concatenate([faces_row[j : j + 1] for j in range(6)], axis=1)
    pick_ref[...] = jnp.where(iota((ROWS, SLOTS), 1).astype(f32) == slots_col, 1.0, 0.0).astype(bf16)
    pick_t_ref[...] = jnp.where(iota((SLOTS, ROWS), 0).astype(f32) == slots_row, 1.0, 0.0).astype(bf16)
    lanes = iota((ROWS, WIDE), 1)
    valid = ((lanes // 32).astype(f32) == codes_col) & (lanes % 32 < FACE_DOFS)
    valid_ref[...] = jnp.where(valid, 1.0, 0.0)

    inside = iota((ELEM_DEV, WIDE), 1) < TRACE_DOFS
    for n, ref in enumerate((load_ref, diag_ref)):
        values = jnp.where(inside, ref[...].reshape(ELEM_DEV, WIDE), 0.0)
        fields_ref[n] = collect(values, pick_t_ref[...], valid_ref[...], place_ref[...])
    send_fields(fields_ref, links, bucket_ref, False)


def send_fields(fields_ref, links, bucket_ref, wide):
    rows = [[message(fields_ref.at[n], links, m) for n in range(2)] for m in range(4)]
    fill = jnp.where(iota((1, 128), 1) == 25, links.clash(), 0.0)
    write_bucket(bucket_ref, fill, links, rows, wide)


def resend_kernel(owned_ref, remote_ref, lower_ref, upper_ref, fields_ref, bucket_ref):
    send_fields(fields_ref, Links(owned_ref, remote_ref, lower_ref, upper_ref), bucket_ref, True)


def sum_rows(x):
    total = x[0:8]
    for at in range(8, x.shape[0], 8):
        total = total + x[at : at + 8]
    return jnp.sum(total, axis=0, keepdims=True)


def total_of(x):
    return jnp.sum(jnp.sum(x, axis=0, keepdims=True), axis=1, keepdims=True)


def apply_and_send(r, z, q, links, fixed, partial_ref, bucket_ref, image_ref, wide):
    schur_ref, pick_ref, pick_t_ref, valid_ref, place_ref = fixed
    x = spread(z, pick_ref[...], valid_ref[...], place_ref[...])
    pad = jnp.zeros((128 - ELEM_DEV, 128), f32)
    head = jnp.concatenate([x[:, 0:128], pad], axis=0).T
    tail = jnp.concatenate([x[:, 128:256], pad], axis=0).T[: TRACE_PAD - 128]
    columns = jnp.concatenate([head, tail], axis=0)
    for e in range(ELEM_DEV):
        image_ref[e : e + 1, :] = jnp.sum(schur_ref[e] * columns[:, e : e + 1], axis=0, keepdims=True)
    images = image_ref[...]
    quad = total_of(x * images)
    own = iota((FACE_DEV, 128), 1) < FACE_DOFS
    rz = total_of(jnp.where(own, r[:FACE_DEV] * z[:FACE_DEV], 0.0))
    zq = total_of(jnp.where(own, z[:FACE_DEV] * q[:FACE_DEV], 0.0))
    partial_ref[...] = collect(images, pick_t_ref[...], valid_ref[...], place_ref[...])
    rows = [[message(partial_ref, links, m)] for m in range(4)]
    lane = iota((1, 128), 1)
    sums = jnp.where(lane == 25, quad, jnp.where(lane == 26, rz, jnp.where(lane == 27, zq, 0.0)))
    write_bucket(bucket_ref, sums, links, rows, wide)


def start_kernel(wide, owned_ref, remote_ref, lower_ref, upper_ref, fields_in_ref, arrived_ref, *refs):
    links = Links(owned_ref, remote_ref, lower_ref, upper_ref)
    fixed, (state_ref, partial_ref, bucket_ref, clash_ref, fields_ref, image_ref) = refs[:5], refs[5:]
    clash_ref[0] = jnp.sum(sum_rows(arrived_ref[...])[:, 25:26])
    fields_ref[...] = fields_in_ref[...]
    for n in range(2):
        settle(fields_ref.at[n], read_bucket(arrived_ref, links, 2, n, wide), links)
    inside = iota((SLOTS, 128), 1) % 32 < FACE_DOFS
    r = jnp.where(inside, fields_ref[0], 0.0)
    diag = jnp.where(inside, fields_ref[1], 1.0)
    zero = jnp.zeros((SLOTS, 128), f32)
    z = r / diag
    state_ref[0] = zero
    state_ref[1] = zero
    state_ref[2] = r
    state_ref[3] = zero
    state_ref[4] = diag
    state_ref[5] = jnp.where(iota((SLOTS, 128), 0) == 0, jnp.inf, 0.0)
    apply_and_send(r, z, zero, links, fixed, partial_ref, bucket_ref, image_ref, wide)


def advance(wide, links, partial_in_ref, arrived_ref, state_ref, work_ref):
    work_ref[...] = partial_in_ref[...]
    settle(work_ref, read_bucket(arrived_ref, links, 1, 0, wide), links)
    sums = sum_rows(arrived_ref[...])
    if wide:
        sums = sums * 0.5
    quad, rz, zq = sums[:, 25:26], sums[:, 26:27], sums[:, 27:28]
    old_rz, old_energy = state_ref[5, 0:1, 0:1], state_ref[5, 1:2, 0:1]
    beta = rz / old_rz
    direction = state_ref[2] / state_ref[4] + beta * state_ref[1]
    image = work_ref[...] + beta * state_ref[3]
    energy = quad + 2.0 * beta * zq + beta * beta * old_energy
    alpha = rz / energy
    trace = state_ref[0] + alpha * direction
    residual = state_ref[2] - alpha * image
    return trace, direction, residual, image, rz, energy


def step_kernel(wide, owned_ref, remote_ref, lower_ref, upper_ref, partial_in_ref, arrived_ref, state_in_ref, *refs):
    links = Links(owned_ref, remote_ref, lower_ref, upper_ref)
    fixed, (state_ref, partial_ref, bucket_ref, work_ref, image_ref) = refs[:5], refs[5:]
    trace, direction, residual, image, rz, energy = advance(
        wide, links, partial_in_ref, arrived_ref, state_in_ref, work_ref
    )
    diag = state_in_ref[4]
    state_ref[0] = trace
    state_ref[1] = direction
    state_ref[2] = residual
    state_ref[3] = image
    state_ref[4] = diag
    state_ref[5] = jnp.where(iota((SLOTS, 128), 0) == 0, rz, energy)
    apply_and_send(
        residual, residual / diag, image, links, fixed, partial_ref, bucket_ref, image_ref, wide
    )


def finish_kernel(
    wide, owned_ref, remote_ref, lower_ref, upper_ref, partial_in_ref, arrived_ref, state_in_ref,
    trace_ref, residual_ref, work_ref,
):
    links = Links(owned_ref, remote_ref, lower_ref, upper_ref)
    trace, _, residual, _, _, _ = advance(wide, links, partial_in_ref, arrived_ref, state_in_ref, work_ref)
    pad = jnp.zeros((128 - FACE_DEV, 128), f32)
    trace_ref[...] = jnp.concatenate([trace[:FACE_DEV], pad], axis=0).T[:FACE_DOFS, :FACE_DEV]
    residual_ref[...] = jnp.concatenate([residual[:FACE_DEV], pad], axis=0).T[:FACE_DOFS, :FACE_DEV]


VMEM = pl.BlockSpec(memory_space=pltpu.VMEM)
SMEM = pl.BlockSpec(memory_space=pltpu.SMEM)
HBM = pl.BlockSpec(memory_space=pltpu.HBM)


def shape(*dims, dtype=f32):
    return jax.ShapeDtypeStruct(dims, dtype)


def call(body, name, scalars, arrays, outs, scratch, specs=None, out_specs=None, grant=12):
    return pl.pallas_call(
        body,
        name=name,
        in_specs=[SMEM] * len(scalars) + (specs or [VMEM] * len(arrays)),
        out_specs=out_specs or [VMEM] * len(outs),
        out_shape=outs,
        scratch_shapes=[pltpu.VMEM(item, f32) if isinstance(item, tuple) else item for item in scratch],
        compiler_params=pltpu.CompilerParams(vmem_limit_bytes=grant << 20),
        interpret=INTERPRET,
    )(*scalars, *arrays)


def on_device(
    basis_mats,
    coeffs,
    element_loads,
    elem_faces,
    orient_codes,
    shared_owned,
    shared_remote,
    lower_peers,
    upper_peers,
):
    axes = ("gx", "gy")
    devices = lax.axis_size("gx") * lax.axis_size("gy")
    links = (shared_owned, shared_remote, lower_peers, upper_peers)
    place = jnp.asarray(place_matrix(), bf16)
    width = CELL_PAD + WIDE

    def exchange_twice(bucket):
        grid = (lax.axis_size("gx"), lax.axis_size("gy"), bucket.shape[0] // devices, 128)
        sent = lax.all_to_all(bucket.reshape(grid), "gx", split_axis=0, concat_axis=0, tiled=True)
        return lax.all_to_all(sent, "gy", split_axis=1, concat_axis=1, tiled=True).reshape(bucket.shape)

    def exchange(bucket):
        parts = bucket.shape[0] // devices
        sent = bucket.reshape(devices, parts, 128) if parts > 1 else bucket
        got = lax.all_to_all(sent, axes, split_axis=0, concat_axis=0, tiled=True)
        return got.reshape(bucket.shape)

    schur, fields, pick, pick_t, valid, bucket = call(
        condense_kernel,
        "condense",
        (coeffs,) + links,
        (pltpu.with_memory_space_constraint(basis_mats, pltpu.HBM), element_loads, elem_faces.T, orient_codes.T, place),
        (
            shape(ELEM_DEV, TRACE_PAD, WIDE),
            shape(2, SLOTS, 128),
            shape(ROWS, SLOTS, dtype=bf16),
            shape(SLOTS, ROWS, dtype=bf16),
            shape(ROWS, WIDE),
            shape(2 * devices, 128),
        ),
        (
            (TERMS, CELL_PAD + TRACE_PAD, width),
            (ELEM_DEV, CELL_PAD, width),
            pltpu.VMEM((3, ELEM_DEV, CELL_PAD, width), bf16),
            (ELEM_DEV, PIVOT, 128),
            (ELEM_DEV, 1, WIDE),
            (ELEM_DEV, 1, WIDE),
            (TERMS, LOCAL_DOFS, LOCAL_DOFS),
            pltpu.SemaphoreType.DMA((TERMS,)),
        ),
        specs=[HBM] + [VMEM] * 4,
        grant=44,
    )
    fixed = (schur, pick, pick_t, valid, place)

    def start(arrived, wide):
        return call(
            lambda *refs: start_kernel(wide, *refs),
            "start_wide" if wide else "start",
            links,
            (fields, arrived) + fixed,
            (shape(6, SLOTS, 128), shape(SLOTS, 128), shape((1 + wide) * devices, 128), shape(1)),
            ((2, SLOTS, 128), (ELEM_DEV, WIDE)),
            out_specs=[VMEM] * 3 + [SMEM],
        )

    def step(state, partial_value, arrived, wide):
        return call(
            lambda *refs: step_kernel(wide, *refs),
            "step_wide" if wide else "step",
            links,
            (partial_value, arrived, state) + fixed,
            (shape(6, SLOTS, 128), shape(SLOTS, 128), shape((1 + wide) * devices, 128)),
            ((SLOTS, 128), (ELEM_DEV, WIDE)),
        )

    def finish(state, partial_value, arrived, wide):
        return tuple(
            call(
                lambda *refs: finish_kernel(wide, *refs),
                "finish_wide" if wide else "finish",
                links,
                (partial_value, arrived, state),
                (shape(FACE_DOFS, FACE_DEV), shape(FACE_DOFS, FACE_DEV)),
                ((SLOTS, 128),),
            )
        )

    def narrow_run(state, partial_value, bucket):
        def body(_, carry):
            state, partial_value, bucket = carry
            return tuple(step(state, partial_value, exchange(bucket), False))

        carry = lax.fori_loop(0, ITERS - 1, body, (state, partial_value, bucket))
        state, partial_value, bucket = carry
        return finish(state, partial_value, exchange(bucket), False)

    def wide_run(state, partial_value, bucket):
        (again,) = call(resend_kernel, "resend", links, (fields,), (shape(4 * devices, 128),), ())
        state, partial_value, bucket, _ = start(exchange_twice(again), True)

        def body(_, carry):
            state, partial_value, bucket = carry
            return tuple(step(state, partial_value, exchange_twice(bucket), True))

        carry = lax.fori_loop(0, ITERS, body, (state, partial_value, bucket))
        return carry[0][0, :FACE_DEV, :FACE_DOFS].T, carry[0][2, :FACE_DEV, :FACE_DOFS].T

    state, partial_value, bucket, clash = start(exchange(bucket), False)
    return lax.cond(clash[0] > 0.0, wide_run, narrow_run, state, partial_value, bucket)


def solution(mesh):
    placed = (
        P(),
        P(("gx", "gy"), None),
        P(("gx", "gy"), None),
        P(("gx", "gy"), None),
        P(("gx", "gy"), None),
        P(("gx", "gy"), None, None),
        P(("gx", "gy"), None, None),
        P(("gx", "gy"), None),
        P(("gx", "gy"), None),
    )
    return jax.shard_map(
        on_device,
        mesh=mesh,
        in_specs=placed,
        out_specs=(P(None, ("gx", "gy")), P(None, ("gx", "gy"))),
        check_vma=False,
    )
```

```python
import jax
import jax.numpy as jnp
import numpy as np
from jax import lax
from jax.experimental import pallas as pl
from jax.experimental.pallas import tpu as pltpu
from jax.sharding import PartitionSpec as P

SIDE = 5
FACE_DOFS = 25
CELL_DOFS = 125
TRACE_DOFS = 150
LOCAL_DOFS = 275
TERMS = 12
ITERS = 4
ELEM_DEV = 16
FACE_DEV = 64
SHARED = 4
REMOTE = 8
SLOTS = FACE_DEV + REMOTE
ROWS = 6 * ELEM_DEV
PIVOT = 16
CELL_PAD = 128
TRACE_PAD = 152
VALID_SLAB = ELEM_DEV
PLACE_SLAB = ELEM_DEV + 1
LOAD_LANE = TRACE_DOFS
WIDE = 256

INTERPRET = False
f32 = jnp.float32
bf16 = jnp.bfloat16


def thirds(x):
    high = x.astype(bf16)
    rest = x - high.astype(f32)
    middle = rest.astype(bf16)
    return high, middle, (rest - middle.astype(f32)).astype(bf16)


def left_parts(parts, axis=0):
    high, middle, low = parts
    return jnp.concatenate([high, high, middle, high, low, middle], axis=axis)


def right_parts(parts):
    high, middle, low = parts
    return jnp.concatenate([high, middle, high, low, high, middle], axis=0)


def product(a, b, contract=0):
    dims = (((contract,), (0,)), ((), ()))
    return lax.dot_general(a, b, dims, preferred_element_type=f32)


def pick_left(mask, x):
    return sum(jnp.dot(mask, part, preferred_element_type=f32) for part in thirds(x))


def pick_right(x, mask, contract=0):
    dims = (((1,), (contract,)), ((), ()))
    return sum(lax.dot_general(part, mask, dims, preferred_element_type=f32) for part in thirds(x))


def orient_table():
    n = SIDE
    table = np.zeros((8, n * n), np.int32)
    for code in range(8):
        for a in range(n):
            for b in range(n):
                a2, b2 = (b, a) if code & 1 else (a, b)
                if code & 2:
                    a2 = n - 1 - a2
                if code & 4:
                    b2 = n - 1 - b2
                table[code, a * n + b] = a2 * n + b2
    return table


def place_matrix():
    table = orient_table()
    place = np.zeros((WIDE, WIDE), np.float32)
    for code in range(8):
        for q in range(FACE_DOFS):
            for j in range(6):
                place[code * 32 + table[code, q], j * FACE_DOFS + q] = 1.0
    return place


def iota(shape, axis):
    return lax.broadcasted_iota(jnp.int32, shape, axis)


def retile(x):
    x = x + pltpu.roll(x, 64, 1)
    return x + pltpu.roll(x, 32, 1)


def spread(field, pick, valid, place):
    rows = pick_left(pick, field)
    rows = jnp.concatenate([rows, rows], axis=1) * valid
    placed = pick_right(rows, place)
    lane = iota((ELEM_DEV, WIDE), 1)
    total = jnp.zeros((ELEM_DEV, WIDE), f32)
    for j in range(6):
        mine = (lane >= j * FACE_DOFS) & (lane < (j + 1) * FACE_DOFS)
        total = jnp.where(mine, placed[j * ELEM_DEV : (j + 1) * ELEM_DEV], total)
    return total


def collect(values, pick_t, valid, place):
    lane = iota((ELEM_DEV, WIDE), 1)
    parts = []
    for j in range(6):
        mine = (lane >= j * FACE_DOFS) & (lane < (j + 1) * FACE_DOFS)
        parts.append(jnp.where(mine, values, 0.0))
    turned = pick_right(jnp.concatenate(parts, axis=0), place, 1) * valid
    summed = pick_left(pick_t, turned)
    return retile(summed[:, :128] + summed[:, 128:])


class Links:
    def __init__(self, owned_ref, remote_ref, lower_ref, upper_ref):
        self.owned, self.remote, self.lower, self.upper = owned_ref, remote_ref, lower_ref, upper_ref

    def peer(self, m):
        return (self.lower if m < 2 else self.upper)[0, m % 2]

    def slot(self, m, k):
        if m < 2:
            return self.owned[0, m, k]
        return FACE_DEV + self.remote[0, m - 2, k]

    def clash(self):
        hits = [jnp.where(self.peer(i) == self.peer(2 + j), 1, 0) for i in range(2) for j in range(2)]
        return jnp.where(hits[0] + hits[1] + hits[2] + hits[3] > 0, 1.0, 0.0)


def message(ref, links, m):
    block = iota((1, 128), 1) // 32
    row = ref[pl.ds(links.slot(m, 0), 1), :]
    for k in range(1, SHARED):
        row = jnp.where(block == k, ref[pl.ds(links.slot(m, k), 1), :], row)
    return row


def settle(ref, incoming, links):
    block = iota((1, 128), 1) // 32
    inside = iota((1, 128), 1) % 32 < FACE_DOFS
    rows = []
    for m in range(4):
        row = jnp.where(inside, incoming[m], 0.0)
        for k in range(SHARED):
            rows.append(jnp.where(block == k, row, 0.0))
    rows = retile(jnp.concatenate(rows, axis=0))
    for m in range(4):
        for k in range(SHARED):
            at = pl.ds(links.slot(m, k), 1)
            ref[at, :] = ref[at, :] + rows[m * SHARED + k : m * SHARED + k + 1]


def write_bucket(out_ref, fill, links, rows, wide):
    count = len(rows[0])
    out_ref[...] = jnp.broadcast_to(fill, out_ref.shape)
    keep = iota((1, 128), 1) % 32 < FACE_DOFS
    for m in range(4):
        start = links.peer(m) * (2 * count if wide else count) + (count * (m // 2) if wide else 0)
        for n in range(count):
            out_ref[pl.ds(start + n, 1), :] = jnp.where(keep, rows[m][n], fill)


def read_bucket(in_ref, links, count, n, wide):
    got = []
    for m in range(4):
        start = links.peer(m) * (2 * count if wide else count) + (count * (1 - m // 2) if wide else 0)
        got.append(in_ref[pl.ds(start + n, 1), :])
    return got


def invert_blocks(x):
    n = PIVOT
    halves = n // 8
    sub = iota((8, 128), 0)
    for k in range(n):
        kh, ks = k // 8, k % 8
        hit = sub == ks
        factors = [jnp.broadcast_to(x[i][kh][ks : ks + 1], (8, 128)) for i in range(n)]
        inv = 1.0 / factors[k]
        lead = [x[k][h] * inv for h in range(halves)]
        lead[kh] = jnp.where(hit, inv, lead[kh])
        for i in range(n):
            if i == k:
                continue
            for h in range(halves):
                old = jnp.where(hit, 0.0, x[i][h]) if h == kh else x[i][h]
                x[i][h] = old - factors[i] * lead[h]
        x[k] = lead
    return x


def condense_kernel(
    owned_ref,
    remote_ref,
    lower_ref,
    upper_ref,
    basis_ref,
    coeffs_in_ref,
    loads_in_ref,
    faces_in_ref,
    codes_in_ref,
    place_in_ref,
    schur_ref,
    fields_ref,
    pick_ref,
    pick_t_ref,
    bucket_ref,
    shifted_ref,
    panel_ref,
    scaled_ref,
    inverse_ref,
    diag_ref,
    load_ref,
    terms_ref,
    coeffs_ref,
    loads_ref,
    faces_ref,
    codes_ref,
    place_ref,
    copies,
    small_copies,
):
    links = Links(owned_ref, remote_ref, lower_ref, upper_ref)
    width = CELL_PAD + WIDE

    small = [
        pltpu.make_async_copy(source, target, small_copies.at[n])
        for n, (source, target) in enumerate(
            (
                (coeffs_in_ref, coeffs_ref),
                (loads_in_ref, loads_ref),
                (faces_in_ref, faces_ref),
                (codes_in_ref, codes_ref),
                (place_in_ref, place_ref),
            )
        )
    ]

    def copy_in(k, part):
        rows = slice(0, 128) if part == 0 else slice(128, LOCAL_DOFS)
        return pltpu.make_async_copy(basis_ref.at[k, rows], terms_ref.at[k, rows], copies.at[part, k])

    small[0].start()
    for k in range(TERMS):
        copy_in(k, 0).start()
    for k in range(TERMS):
        copy_in(k, 1).start()
    for copy in small[1:]:
        copy.start()

    def shift_cells(k, carry):
        copy_in(k, 0).wait()
        shifted_ref[k, 0:128, 0:125] = terms_ref[k, 0:128, 0:125]
        shifted_ref[k, 0:128, 125:128] = jnp.zeros((128, 3), f32)
        shifted_ref[k, 0:128, 128:278] = terms_ref[k, 0:128, 125:275]
        shifted_ref[k, 0:128, 278:384] = jnp.zeros((128, 106), f32)
        return carry

    def shift_traces(k, carry):
        copy_in(k, 1).wait()
        shifted_ref[k, 128:278, 128:278] = terms_ref[k, 125:275, 125:275]
        shifted_ref[k, 128:280, 278:384] = jnp.zeros((152, 106), f32)
        return carry

    small[0].wait()
    lax.fori_loop(0, TERMS, shift_cells, 0)

    def cell_rows(g, carry):
        at = pl.ds(pl.multiple_of(g * 8, 8), 8)
        terms = [shifted_ref[k, at, :] for k in range(TERMS)]
        for e in range(ELEM_DEV):
            total = coeffs_ref[e, 0] * terms[0]
            for k in range(1, TERMS):
                total = total + coeffs_ref[e, k] * terms[k]
            panel_ref[e, at, :] = total
        return carry

    lax.fori_loop(0, CELL_PAD // 8, cell_rows, 0)
    lax.fori_loop(0, TERMS, shift_traces, 0)

    def trace_rows(g, carry):
        at = pl.ds(pl.multiple_of(g * 8, 8), 8)
        source = pl.ds(pl.multiple_of(CELL_PAD + g * 8, 8), 8)
        terms = [shifted_ref[k, source, CELL_PAD:] for k in range(TERMS)]
        for e in range(ELEM_DEV):
            total = coeffs_ref[e, 0] * terms[0]
            for k in range(1, TERMS):
                total = total + coeffs_ref[e, k] * terms[k]
            schur_ref[e, at, :] = total
        return carry

    lax.fori_loop(0, TRACE_PAD // 8, trace_rows, 0)
    for copy in small[1:]:
        copy.wait()

    unit = (iota((3, width), 1) == iota((3, width), 0) + CELL_DOFS).astype(f32)
    load_lane = iota((CELL_PAD, 128), 1) == (CELL_PAD + LOAD_LANE) % 128
    pad = jnp.zeros((128 - ELEM_DEV, 128), f32)
    load_cols = jnp.concatenate([loads_ref[:, 0:128], pad], axis=0).T
    for e in range(ELEM_DEV):
        column = jnp.broadcast_to(load_cols[:, e : e + 1], (CELL_PAD, 128))
        panel_ref[e, :, 256:384] = jnp.where(load_lane, column, panel_ref[e, :, 256:384])
        panel_ref[e, CELL_DOFS:CELL_PAD, :] = unit
        schur_ref[e, LOAD_LANE:TRACE_PAD, :] = jnp.zeros((TRACE_PAD - LOAD_LANE, WIDE), f32)
        schur_ref[e, LOAD_LANE : LOAD_LANE + 1, 0:TRACE_DOFS] = loads_ref[e : e + 1, CELL_DOFS:LOCAL_DOFS]

    group = iota((ELEM_DEV, 128), 1) // PIVOT
    scaled_ref[...] = jnp.zeros(scaled_ref.shape, bf16)

    def folded(x):
        return x[0:PIVOT] + (x[PIVOT : 2 * PIVOT] + x[2 * PIVOT : 3 * PIVOT])

    for step in range(CELL_PAD // PIVOT):
        base = step * PIVOT
        own = slice(base, base + PIVOT)
        if step > 0:
            for e in range(ELEM_DEV):
                depth = 32 if base <= 32 else 64 if base <= 64 else 128
                left = panel_ref[e, 0:base, 0:128].T[own]
                if base < 128:
                    left = jnp.concatenate([left, jnp.zeros((PIVOT, 128 - base), f32)], axis=1)
                if depth == 128:
                    left = jnp.concatenate([left, left, left], axis=1)
                elif depth == 64:
                    left = jnp.concatenate([left + pltpu.roll(left, 64, 1), left], axis=1)
                else:
                    left = left + pltpu.roll(left, 32, 1) + pltpu.roll(left, 64, 1)
                lane = iota(left.shape, 1)
                stacked = jnp.concatenate(
                    [
                        jnp.where(lane < (3 - n) * depth, part.astype(f32), 0.0).astype(bf16)
                        for n, part in enumerate(thirds(left))
                    ],
                    axis=0,
                )[:, 0 : 3 * depth]
                right = jnp.concatenate([scaled_ref[n, e, 0:depth, :] for n in range(3)], axis=0)
                panel_ref[e, own, :] = panel_ref[e, own, :] - folded(product(stacked, right, 1))
        x = []
        for half in range(PIVOT // 8):
            packed = jnp.zeros((ELEM_DEV, 128), f32)
            for s in range(8):
                slab = panel_ref[:, base + half * 8 + s, 0:128]
                turn = (s * PIVOT - base) % 128
                if turn:
                    slab = pltpu.roll(slab, turn, 1)
                packed = jnp.where(group == s, slab, packed)
            tall = jnp.concatenate([packed, jnp.zeros((128 - ELEM_DEV, 128), f32)], axis=0).T
            for s in range(8):
                x.append([tall[s * PIVOT + 8 * h : s * PIVOT + 8 * h + 8] for h in range(PIVOT // 8)])
        x = invert_blocks(x)
        for half in range(PIVOT // 8):
            tall = jnp.concatenate([v for s in range(8) for v in x[half * 8 + s]], axis=0)
            packed = tall.T[:ELEM_DEV]
            for s in range(8):
                first, second, third = (
                    pltpu.roll(packed, (t - s) * PIVOT % 128, 1) if (t - s) % 8 else packed for t in range(3)
                )
                inverse_ref[:, half * 8 + s, :] = jnp.where(group == 0, first, jnp.where(group == 1, second, third))
        for e in range(ELEM_DEV):
            top = panel_ref[e, own, :]
            parts = thirds(inverse_ref[e])
            stacked = jnp.concatenate(
                [
                    jnp.where(group < 3 - n, part.astype(f32), 0.0).astype(bf16)
                    for n, part in enumerate(parts)
                ],
                axis=0,
            )
            right = jnp.concatenate(thirds(top), axis=0)
            scaled = thirds(folded(product(stacked[:, 0 : 3 * PIVOT], right, 1)))
            for n in range(3):
                scaled_ref[n, e, own, :] = scaled[n]

    diagonal = iota((TRACE_PAD, WIDE), 0) == iota((TRACE_PAD, WIDE), 1)

    def finish(e, carry):
        left = panel_ref[e, :, CELL_PAD : CELL_PAD + WIDE].T[:TRACE_PAD]
        right = right_parts([scaled_ref[n, e, :, CELL_PAD : CELL_PAD + WIDE] for n in range(3)])
        block = schur_ref[e] - product(left_parts(thirds(left), 1), right, 1)
        schur_ref[e] = block
        at = pl.ds(e, 1)
        diag_ref[at] = jnp.sum(jnp.where(diagonal, block, 0.0), axis=0, keepdims=True)[None]
        load_ref[at] = block[LOAD_LANE : LOAD_LANE + 1][None]
        return carry

    lax.fori_loop(0, ELEM_DEV, finish, 0, unroll=4)

    faces_row = faces_ref[...].astype(f32)
    square = jnp.zeros((122, 128), f32)
    fill = jnp.zeros((6, 128 - ELEM_DEV), f32)
    faces_t = jnp.concatenate([jnp.concatenate([faces_row, fill], axis=1), square], axis=0).T
    codes_t = jnp.concatenate([jnp.concatenate([codes_ref[...].astype(f32), fill], axis=1), square], axis=0).T
    slots_col = jnp.concatenate([faces_t[:ELEM_DEV, j : j + 1] for j in range(6)], axis=0)
    codes_col = jnp.concatenate([codes_t[:ELEM_DEV, j : j + 1] for j in range(6)], axis=0)
    slots_row = jnp.concatenate([faces_row[j : j + 1] for j in range(6)], axis=1)
    pick_ref[...] = jnp.where(iota((ROWS, SLOTS), 1).astype(f32) == slots_col, 1.0, 0.0).astype(bf16)
    pick_t_ref[...] = jnp.where(iota((SLOTS, ROWS), 0).astype(f32) == slots_row, 1.0, 0.0).astype(bf16)
    lanes = iota((ROWS, WIDE), 1)
    valid = ((lanes // 32).astype(f32) == codes_col) & (lanes % 32 < FACE_DOFS)
    schur_ref[VALID_SLAB, 0:ROWS] = jnp.where(valid, 1.0, 0.0)
    schur_ref[PLACE_SLAB, 0:128] = place_ref[0:128].astype(f32)
    schur_ref[PLACE_SLAB + 1, 0:128] = place_ref[128:256].astype(f32)

    inside = iota((ELEM_DEV, WIDE), 1) < TRACE_DOFS
    for n, ref in enumerate((load_ref, diag_ref)):
        values = jnp.where(inside, ref[...].reshape(ELEM_DEV, WIDE), 0.0)
        fields_ref[n] = collect(values, pick_t_ref[...], schur_ref[VALID_SLAB, 0:ROWS], place_ref[...])
    send_fields(fields_ref, links, bucket_ref, False)


def send_fields(fields_ref, links, bucket_ref, wide):
    rows = [[message(fields_ref.at[n], links, m) for n in range(2)] for m in range(4)]
    fill = jnp.where(iota((1, 128), 1) == 25, links.clash(), 0.0)
    write_bucket(bucket_ref, fill, links, rows, wide)


def resend_kernel(owned_ref, remote_ref, lower_ref, upper_ref, fields_ref, bucket_ref):
    send_fields(fields_ref, Links(owned_ref, remote_ref, lower_ref, upper_ref), bucket_ref, True)


def sum_rows(x):
    total = x[0:8]
    for at in range(8, x.shape[0], 8):
        total = total + x[at : at + 8]
    return jnp.sum(total, axis=0, keepdims=True)


def total_of(x):
    return jnp.sum(jnp.sum(x, axis=0, keepdims=True), axis=1, keepdims=True)


def apply_and_send(r, z, q, links, fixed, partial_ref, bucket_ref, image_ref, wide):
    schur_ref, pick_ref, pick_t_ref = fixed
    valid = schur_ref[VALID_SLAB, 0:ROWS]
    place = jnp.concatenate([schur_ref[PLACE_SLAB + n, 0:128].astype(bf16) for n in range(2)], axis=0)
    x = spread(z, pick_ref[...], valid, place)
    pad = jnp.zeros((128 - ELEM_DEV, 128), f32)
    head = jnp.concatenate([x[:, 0:128], pad], axis=0).T
    tail = jnp.concatenate([x[:, 128:256], pad], axis=0).T[: TRACE_PAD - 128]
    columns = jnp.concatenate([head, tail], axis=0)
    for e in range(ELEM_DEV):
        image_ref[e : e + 1, :] = jnp.sum(schur_ref[e] * columns[:, e : e + 1], axis=0, keepdims=True)
    images = image_ref[...]
    quad = total_of(x * images)
    own = iota((FACE_DEV, 128), 1) < FACE_DOFS
    rz = total_of(jnp.where(own, r[:FACE_DEV] * z[:FACE_DEV], 0.0))
    zq = total_of(jnp.where(own, z[:FACE_DEV] * q[:FACE_DEV], 0.0))
    partial_ref[...] = collect(images, pick_t_ref[...], valid, place)
    rows = [[message(partial_ref, links, m)] for m in range(4)]
    lane = iota((1, 128), 1)
    sums = jnp.where(lane == 25, quad, jnp.where(lane == 26, rz, jnp.where(lane == 27, zq, 0.0)))
    write_bucket(bucket_ref, sums, links, rows, wide)


def start_kernel(wide, owned_ref, remote_ref, lower_ref, upper_ref, fields_in_ref, arrived_ref, *refs):
    links = Links(owned_ref, remote_ref, lower_ref, upper_ref)
    fixed, (state_ref, partial_ref, bucket_ref, clash_ref, fields_ref, image_ref) = refs[:3], refs[3:]
    clash_ref[0] = jnp.sum(sum_rows(arrived_ref[...])[:, 25:26])
    fields_ref[...] = fields_in_ref[...]
    for n in range(2):
        settle(fields_ref.at[n], read_bucket(arrived_ref, links, 2, n, wide), links)
    inside = iota((SLOTS, 128), 1) % 32 < FACE_DOFS
    r = jnp.where(inside, fields_ref[0], 0.0)
    diag = jnp.where(inside, fields_ref[1], 1.0)
    zero = jnp.zeros((SLOTS, 128), f32)
    z = r / diag
    state_ref[0] = zero
    state_ref[1] = zero
    state_ref[2] = r
    state_ref[3] = zero
    state_ref[4] = diag
    state_ref[5] = jnp.where(iota((SLOTS, 128), 0) == 0, jnp.inf, 0.0)
    apply_and_send(r, z, zero, links, fixed, partial_ref, bucket_ref, image_ref, wide)


def advance(wide, links, partial_in_ref, arrived_ref, state_ref, work_ref):
    work_ref[...] = partial_in_ref[...]
    settle(work_ref, read_bucket(arrived_ref, links, 1, 0, wide), links)
    sums = sum_rows(arrived_ref[...])
    if wide:
        sums = sums * 0.5
    quad, rz, zq = sums[:, 25:26], sums[:, 26:27], sums[:, 27:28]
    old_rz, old_energy = state_ref[5, 0:1, 0:1], state_ref[5, 1:2, 0:1]
    beta = rz / old_rz
    direction = state_ref[2] / state_ref[4] + beta * state_ref[1]
    image = work_ref[...] + beta * state_ref[3]
    energy = quad + 2.0 * beta * zq + beta * beta * old_energy
    alpha = rz / energy
    trace = state_ref[0] + alpha * direction
    residual = state_ref[2] - alpha * image
    return trace, direction, residual, image, rz, energy


def step_kernel(wide, owned_ref, remote_ref, lower_ref, upper_ref, partial_in_ref, arrived_ref, state_in_ref, *refs):
    links = Links(owned_ref, remote_ref, lower_ref, upper_ref)
    fixed, (state_ref, partial_ref, bucket_ref, work_ref, image_ref) = refs[:3], refs[3:]
    trace, direction, residual, image, rz, energy = advance(
        wide, links, partial_in_ref, arrived_ref, state_in_ref, work_ref
    )
    diag = state_in_ref[4]
    state_ref[0] = trace
    state_ref[1] = direction
    state_ref[2] = residual
    state_ref[3] = image
    state_ref[4] = diag
    state_ref[5] = jnp.where(iota((SLOTS, 128), 0) == 0, rz, energy)
    apply_and_send(
        residual, residual / diag, image, links, fixed, partial_ref, bucket_ref, image_ref, wide
    )


def finish_kernel(
    wide, owned_ref, remote_ref, lower_ref, upper_ref, partial_in_ref, arrived_ref, state_in_ref,
    trace_ref, residual_ref, work_ref,
):
    links = Links(owned_ref, remote_ref, lower_ref, upper_ref)
    trace, _, residual, _, _, _ = advance(wide, links, partial_in_ref, arrived_ref, state_in_ref, work_ref)
    pad = jnp.zeros((128 - FACE_DEV, 128), f32)
    trace_ref[...] = jnp.concatenate([trace[:FACE_DEV], pad], axis=0).T[:FACE_DOFS, :FACE_DEV]
    residual_ref[...] = jnp.concatenate([residual[:FACE_DEV], pad], axis=0).T[:FACE_DOFS, :FACE_DEV]


VMEM = pl.BlockSpec(memory_space=pltpu.VMEM)
SMEM = pl.BlockSpec(memory_space=pltpu.SMEM)
HBM = pl.BlockSpec(memory_space=pltpu.HBM)


def shape(*dims, dtype=f32):
    return jax.ShapeDtypeStruct(dims, dtype)


def kept(*dims, dtype=f32):
    return shape(*dims, dtype=dtype) if INTERPRET else pltpu.VMEM(dims, dtype)


def call(body, name, scalars, arrays, outs, scratch, specs=None, out_specs=None, grant=4):
    return pl.pallas_call(
        body,
        name=name,
        in_specs=[SMEM] * len(scalars) + (specs or [VMEM] * len(arrays)),
        out_specs=out_specs or [VMEM] * len(outs),
        out_shape=outs,
        scratch_shapes=[pltpu.VMEM(item, f32) if isinstance(item, tuple) else item for item in scratch],
        compiler_params=pltpu.CompilerParams(vmem_limit_bytes=grant << 20),
        interpret=INTERPRET,
    )(*scalars, *arrays)


def on_device(
    basis_mats,
    coeffs,
    element_loads,
    elem_faces,
    orient_codes,
    shared_owned,
    shared_remote,
    lower_peers,
    upper_peers,
):
    axes = ("gx", "gy")
    devices = lax.axis_size("gx") * lax.axis_size("gy")
    links = (shared_owned, shared_remote, lower_peers, upper_peers)
    place = jnp.asarray(place_matrix(), bf16)
    width = CELL_PAD + WIDE

    def exchange_twice(bucket):
        grid = (lax.axis_size("gx"), lax.axis_size("gy"), bucket.shape[0] // devices, 128)
        sent = lax.all_to_all(bucket.reshape(grid), "gx", split_axis=0, concat_axis=0, tiled=True)
        return lax.all_to_all(sent, "gy", split_axis=1, concat_axis=1, tiled=True).reshape(bucket.shape)

    def exchange(bucket):
        parts = bucket.shape[0] // devices
        sent = bucket.reshape(devices, parts, 128) if parts > 1 else bucket
        got = lax.all_to_all(sent, axes, split_axis=0, concat_axis=0, tiled=True)
        return got.reshape(bucket.shape)

    def raw(array):
        return pltpu.with_memory_space_constraint(array, pltpu.HBM)

    schur, fields, pick, pick_t, bucket = call(
        condense_kernel,
        "condense",
        links,
        (raw(basis_mats), raw(coeffs), raw(element_loads), raw(elem_faces.T), raw(orient_codes.T), raw(place)),
        (
            kept(ELEM_DEV + 3, TRACE_PAD, WIDE),
            kept(2, SLOTS, 128),
            kept(ROWS, SLOTS, dtype=bf16),
            kept(SLOTS, ROWS, dtype=bf16),
            shape(2 * devices, 128) if INTERPRET else pltpu.HBM((2 * devices, 128), f32),
        ),
        (
            (TERMS, CELL_PAD + TRACE_PAD, width),
            (ELEM_DEV, CELL_PAD, width),
            pltpu.VMEM((3, ELEM_DEV, CELL_PAD, width), bf16),
            (ELEM_DEV, PIVOT, 128),
            (ELEM_DEV, 1, WIDE),
            (ELEM_DEV, 1, WIDE),
            (TERMS, LOCAL_DOFS, LOCAL_DOFS),
            pltpu.SMEM((ELEM_DEV, TERMS), f32),
            (ELEM_DEV, LOCAL_DOFS),
            pltpu.VMEM((6, ELEM_DEV), jnp.int32),
            pltpu.VMEM((6, ELEM_DEV), jnp.int32),
            pltpu.VMEM((WIDE, WIDE), bf16),
            pltpu.SemaphoreType.DMA((2, TERMS)),
            pltpu.SemaphoreType.DMA((5,)),
        ),
        specs=[HBM] * 6,
        grant=28,
    )
    fixed = (schur, pick, pick_t)

    def start(arrived, wide):
        return call(
            lambda *refs: start_kernel(wide, *refs),
            "start_wide" if wide else "start",
            links,
            (fields, arrived) + fixed,
            (kept(6, SLOTS, 128), kept(SLOTS, 128), shape((1 + wide) * devices, 128), shape(1)),
            ((2, SLOTS, 128), (ELEM_DEV, WIDE)),
            out_specs=[VMEM] * 3 + [SMEM],
        )

    def step(state, partial_value, arrived, wide):
        return call(
            lambda *refs: step_kernel(wide, *refs),
            "step_wide" if wide else "step",
            links,
            (partial_value, arrived, state) + fixed,
            (kept(6, SLOTS, 128), kept(SLOTS, 128), shape((1 + wide) * devices, 128)),
            ((SLOTS, 128), (ELEM_DEV, WIDE)),
        )

    def finish(state, partial_value, arrived, wide):
        return tuple(
            call(
                lambda *refs: finish_kernel(wide, *refs),
                "finish_wide" if wide else "finish",
                links,
                (partial_value, arrived, state),
                (shape(FACE_DOFS, FACE_DEV), shape(FACE_DOFS, FACE_DEV)),
                ((SLOTS, 128),),
            )
        )

    def narrow_run(state, partial_value, bucket):
        def body(_, carry):
            state, partial_value, bucket = carry
            return tuple(step(state, partial_value, exchange(bucket), False))

        carry = lax.fori_loop(0, ITERS - 1, body, (state, partial_value, bucket))
        state, partial_value, bucket = carry
        return finish(state, partial_value, exchange(bucket), False)

    def wide_run(state, partial_value, bucket):
        (again,) = call(resend_kernel, "resend", links, (fields,), (shape(4 * devices, 128),), ())
        state, partial_value, bucket, _ = start(exchange_twice(again), True)

        def body(_, carry):
            state, partial_value, bucket = carry
            return tuple(step(state, partial_value, exchange_twice(bucket), True))

        carry = lax.fori_loop(0, ITERS, body, (state, partial_value, bucket))
        return carry[0][0, :FACE_DEV, :FACE_DOFS].T, carry[0][2, :FACE_DEV, :FACE_DOFS].T

    state, partial_value, bucket, clash = start(exchange(bucket), False)
    return lax.cond(clash[0] > 0.0, wide_run, narrow_run, state, partial_value, bucket)


def solution(mesh):
    placed = (
        P(),
        P(("gx", "gy"), None),
        P(("gx", "gy"), None),
        P(("gx", "gy"), None),
        P(("gx", "gy"), None),
        P(("gx", "gy"), None, None),
        P(("gx", "gy"), None, None),
        P(("gx", "gy"), None),
        P(("gx", "gy"), None),
    )
    return jax.shard_map(
        on_device,
        mesh=mesh,
        in_specs=placed,
        out_specs=(P(None, ("gx", "gy")), P(None, ("gx", "gy"))),
        check_vma=False,
    )
```
